32 devices in a mesh: gx: 8 (over z, x), gy: 4 (over y, core).
Axes of the slice: x: 2, y: 2, z: 4, core: 2. Of those that a mesh axis runs over, the one named last changes fastest.
Arguments:
- populations: float32 [19, 48, 32, 128], P(None, 'gx', 'gy'), may hold values from 0.03 to 0.06
- cell_mass: float32 [48, 32, 128], P('gx', 'gy'), may hold values from 0.05 to 1
- cell_flags: int32 [48, 32, 128], P('gx', 'gy'), may hold values from 0 to 2
- bubble: int32 [48, 32, 128], P('gx', 'gy'), may hold values from 0 to 95, as said below
- conversion: int32 [48, 32, 128], P('gx', 'gy'), may hold values 0 or 1
- rest_volume: float32 [96], replicated, may hold values from 256 to 2048
Outputs:
- relaxed_populations: float32 [19, 48, 32, 128], P(None, 'gx', 'gy')
- new_mass: float32 [48, 32, 128], P('gx', 'gy')
- gas_density: float32 [96], replicated
The draws below stay inside these ranges and needn't reach their ends.
Inputs may be any that keep to these rules, and one draw needn't show every extreme that they name: `cell_flags`: 0 gas, 1 interface, 2 liquid. The bubble that a gas or interface cell belongs to; unused for liquid cells. `conversion`: 1 marks an interface cell that becomes liquid in this step; unused for other cells.
All inputs are finite; a program needn't handle non-finite values. No bound on the sum of `conversion` on one device may be relied on, other than what follows from the above.
Results may differ from the reference program's by a relative error of at most 0.0003.
Values sent between devices are 32-bit elements; how exact they have to be, the bound alone decides.
No kernel may reach another device: no remote copies, remote signals or barrier semaphores. Data moves between devices by JAX's collectives and lax.ppermute only.
A program may use at most 64 MiB of HBM per device.

```python
import math
import jax
import jax.numpy as jnp
import numpy as np
from jax import lax

CX = 6
CY = 8
NZ = 128
BUB_DEV = 3
NX = 48
NY = 32
BUBBLES = 96


def draw_bubble(key, part):
    shifts = jax.random.randint(jax.random.fold_in(key, 11), (3,), 0, 1 << 20, dtype=jnp.int32)
    height_region = (jnp.arange(NX, dtype=jnp.int32) + shifts[0] % NX) % NX // CX
    section_region = (jnp.arange(NY, dtype=jnp.int32) + shifts[1] % NY) % NY // CY
    depth_region = (jnp.arange(NZ, dtype=jnp.int32) + shifts[2] % NZ) % NZ * BUB_DEV // NZ
    region = (height_region[:, None, None] * (NY // CY) + section_region[None, :, None]) * BUB_DEV + depth_region[None, None, :]
    labelling = jax.random.permutation(jax.random.fold_in(key, 23), BUBBLES).astype(jnp.int32)
    boxed = jnp.take(labelling, region)
    scattered = jax.random.randint(jax.random.fold_in(key, 37), (NX, NY, NZ), 0, BUBBLES, dtype=jnp.int32)
    picked = jax.random.randint(jax.random.fold_in(key, 41), (NX, NY, NZ), 0, 4, dtype=jnp.int32) == 0
    return jnp.where(picked, scattered, boxed).astype(jnp.int32)


def place_ends(entries, key, least, largest):
    dims = entries.shape
    spot = [jax.random.randint(jax.random.fold_in(key, axis), (), 0, dims[axis]) for axis in range(len(dims))]
    entries = entries.at[tuple(spot)].set(least)
    longest = dims.index(max(dims))
    spot[longest] = (spot[longest] + 1) % dims[longest]
    return entries.at[tuple(spot)].set(largest)


def level_of(rng, dims, split, smallest, largest):
    level = 1.0
    for position, shards_of in split:
        steps = jax.random.uniform(jax.random.fold_in(jax.random.fold_in(rng, 6), position), (shards_of,), jnp.float32, smallest / len(split), largest / len(split))
        level = level * jnp.repeat(jnp.exp(steps), dims[position] // shards_of).reshape((-1,) + (1,) * (len(dims) - 1 - position))
    return level


def setup_inputs(seed: int = 0) -> dict:
    keys = jax.random.split(jax.random.key(seed), 7)
    return {
        "populations": jnp.clip(0.03 + 0.03 * jax.random.uniform(keys[0], (19, NX, NY, NZ), jnp.float32) ** level_of(keys[0], (19, NX, NY, NZ), ((1, 8), (2, 4)), -0.2, 0.2), 0.03, 0.06),
        "cell_mass": jnp.clip(0.05 + 0.95 * jax.random.uniform(keys[1], (NX, NY, NZ), jnp.float32) ** level_of(keys[1], (NX, NY, NZ), ((0, 8), (1, 4)), -0.2, 0.2), 0.05, 1.0),
        "cell_flags": place_ends(jax.random.randint(keys[2], (NX, NY, NZ), 0, 3), jax.random.fold_in(keys[2], 1), 0, 2).astype(jnp.int32),
        "bubble": draw_bubble(jax.random.fold_in(keys[6], 71), 0),
        "conversion": place_ends((jax.random.randint(keys[4], (NX, NY, NZ), 0, 4) < 1).astype(jnp.int32), jax.random.fold_in(keys[4], 1), 0, 1),
        "rest_volume": jnp.clip(jnp.exp(jax.random.uniform(keys[5], (BUBBLES,), jnp.float32, math.log(256.0), math.log(2048.0))), 256.0, 2048.0),
    }


VELOCITIES = np.array([[0, 0, 0], [1, 0, 0], [-1, 0, 0], [0, 1, 0], [0, -1, 0], [0, 0, 1], [0, 0, -1],
                       [1, 1, 0], [-1, -1, 0], [1, -1, 0], [-1, 1, 0], [1, 0, 1], [-1, 0, -1],
                       [1, 0, -1], [-1, 0, 1], [0, 1, 1], [0, -1, -1], [0, 1, -1], [0, -1, 1]])
OPPOSITE = np.array([0, 2, 1, 4, 3, 6, 5, 8, 7, 10, 9, 12, 11, 14, 13, 16, 15, 18, 17])
WEIGHTS = np.array([1.0 / 3.0] + [1.0 / 18.0] * 6 + [1.0 / 36.0] * 12)
RELAX = 1.0 / 0.6
AMBIENT = 2.0


def moments(populations):
    density = jnp.sum(populations, axis=0)
    lattice = jnp.asarray(VELOCITIES.T, jnp.float32)
    flux = jnp.einsum("kq,qxyz->kxyz", lattice, populations, precision=lax.Precision.HIGHEST)
    return density, flux / density[None]


def unit_equilibrium(velocity):
    lattice = jnp.asarray(VELOCITIES, jnp.float32)
    project = jnp.einsum("qk,kxyz->qxyz", lattice, velocity, precision=lax.Precision.HIGHEST)
    speed = jnp.sum(velocity * velocity, axis=0)
    weights = jnp.asarray(WEIGHTS, jnp.float32)[:, None, None, None]
    return weights * (1.0 + 3.0 * project + 4.5 * project * project - 1.5 * speed[None])


def window(layer, lane, extent_rows, extent_cols):
    offset_rows, offset_cols, offset_depth = (int(value) for value in VELOCITIES[lane])
    begin_rows, begin_cols = 1 - offset_rows, 1 - offset_cols
    return jnp.roll(layer[begin_rows:begin_rows + extent_rows, begin_cols:begin_cols + extent_cols], offset_depth, axis=2)


def domain(inside_rows, inside_cols, lane, extent_rows, extent_cols):
    begin_rows, begin_cols = 1 - int(VELOCITIES[lane][0]), 1 - int(VELOCITIES[lane][1])
    return (inside_rows[begin_rows:begin_rows + extent_rows][:, None, None]
            & inside_cols[begin_cols:begin_cols + extent_cols][None, :, None])


def pull_cells(padded, inside_rows, inside_cols, populations, fraction):
    extent_rows, extent_cols = populations.shape[1], populations.shape[2]
    pulled = [populations[0]]
    gas_side = [jnp.zeros(populations.shape[1:], jnp.bool_)]
    mass_flux = jnp.zeros(populations.shape[1:], jnp.float32)
    targets = jnp.zeros(populations.shape[1:], jnp.float32)
    for lane in range(1, 19):
        source = window(padded[lane], lane, extent_rows, extent_cols)
        source_fraction = window(padded[19], lane, extent_rows, extent_cols)
        source_status = window(padded[20], lane, extent_rows, extent_cols)
        in_domain = domain(inside_rows, inside_cols, lane, extent_rows, extent_cols)
        source_flag = jnp.where(source_status > 2.5, source_status - 3.0, source_status)
        bounced = populations[int(OPPOSITE[lane])]
        pulled.append(jnp.where(in_domain, source, bounced))
        gas_side.append(in_domain & (source_flag < 0.5))
        weight = jnp.where(in_domain & (source_flag > 1.5), 1.0,
                           jnp.where(in_domain & (source_flag > 0.5), 0.5 * (fraction + source_fraction), 0.0))
        mass_flux = mass_flux + weight * (source - bounced)
        targets = targets + jnp.where(in_domain & (jnp.abs(source_status - 1.0) < 0.5), 1.0, 0.0)
    return jnp.stack(pulled), jnp.stack(gas_side), mass_flux, targets


def settle_cells(pulled, gas_side, populations, velocity, local_gas, cell_mass, cell_flags, conversion, mass_flux, targets):
    unit = unit_equilibrium(velocity)
    paired = unit + unit[OPPOSITE]
    bounced = populations[OPPOSITE]
    wetted = cell_flags > 0
    passed = jnp.where(gas_side, local_gas[None] * paired - bounced, pulled)
    passed = jnp.where(wetted[None], passed, populations)
    moved_density, moved_velocity = moments(passed)
    relaxed = passed - RELAX * (passed - moved_density[None] * unit_equilibrium(moved_velocity))
    relaxed = jnp.where(wetted[None], relaxed, populations)
    filling = (cell_flags == 1) & (conversion == 1)
    updated = jnp.where(cell_flags == 1, cell_mass + mass_flux, jnp.where(cell_flags == 2, moved_density, cell_mass))
    portion = jnp.where(filling, (updated - moved_density) / jnp.maximum(targets, 1.0), 0.0)
    updated = jnp.where(filling, moved_density, updated)
    return relaxed, updated, portion


def collect_spill(padded_portion, extent_rows, extent_cols):
    gained = jnp.zeros((extent_rows, extent_cols, padded_portion.shape[2]), jnp.float32)
    for lane in range(1, 19):
        gained = gained + window(padded_portion, lane, extent_rows, extent_cols)
    return gained


def reference(populations, cell_mass, cell_flags, bubble, conversion, rest_volume):
    density, velocity = moments(populations)
    fraction = jnp.clip(cell_mass / density, 0.0, 1.0)
    status = jnp.where((cell_flags == 1) & (conversion == 1), 4, cell_flags).astype(jnp.float32)
    contribution = jnp.where(cell_flags == 0, 1.0, jnp.where(cell_flags == 1, 1.0 - fraction, 0.0))
    volume = jax.ops.segment_sum(contribution.reshape(-1), bubble.reshape(-1), num_segments=BUBBLES)
    gas_density = AMBIENT + rest_volume / jnp.maximum(volume, 1.0)
    local_gas = jnp.take(gas_density, bubble)
    channels = jnp.concatenate([populations, fraction[None], status[None]], axis=0)
    padded = jnp.pad(channels, ((0, 0), (1, 1), (1, 1), (0, 0)))
    inside_rows = jnp.pad(jnp.ones((NX,), jnp.bool_), 1)
    inside_cols = jnp.pad(jnp.ones((NY,), jnp.bool_), 1)
    pulled, gas_side, mass_flux, targets = pull_cells(padded, inside_rows, inside_cols, populations, fraction)
    relaxed, updated, portion = settle_cells(pulled, gas_side, populations, velocity, local_gas,
                                             cell_mass, cell_flags, conversion, mass_flux, targets)
    padded_portion = jnp.pad(portion, ((1, 1), (1, 1), (0, 0)))
    gained = collect_spill(padded_portion, NX, NY)
    receiver = (cell_flags == 1) & (conversion == 0)
    new_mass = jnp.where(receiver, updated + gained, updated)
    return relaxed, new_mass, gas_density
```

```python
import functools

import jax
import jax.numpy as jnp
import numpy as np
from jax import lax
from jax.experimental import pallas as pl
from jax.experimental.pallas import tpu as pltpu
from jax.sharding import PartitionSpec as P

VELOCITIES = np.array(
    [
        [0, 0, 0],
        [1, 0, 0],
        [-1, 0, 0],
        [0, 1, 0],
        [0, -1, 0],
        [0, 0, 1],
        [0, 0, -1],
        [1, 1, 0],
        [-1, -1, 0],
        [1, -1, 0],
        [-1, 1, 0],
        [1, 0, 1],
        [-1, 0, -1],
        [1, 0, -1],
        [-1, 0, 1],
        [0, 1, 1],
        [0, -1, -1],
        [0, 1, -1],
        [0, -1, 1],
    ]
)
OPPOSITE = [0, 2, 1, 4, 3, 6, 5, 8, 7, 10, 9, 12, 11, 14, 13, 16, 15, 18, 17]
WEIGHTS = [1.0 / 3.0] + [1.0 / 18.0] * 6 + [1.0 / 36.0] * 12
RELAX = 1.0 / 0.6
AMBIENT = 2.0
LANES = 19
MASS, FRAC, CODE, BUB = 19, 20, 21, 22
CHANNELS = 23
WALL, GAS, FACE, LIQUID, FILLING = 0.0, 1.0, 2.0, 3.0, 5.0


def heading(axis, sign):
    return [q for q in range(LANES) if VELOCITIES[q][axis] == sign]


def heading_both(rows, cols):
    return [q for q in range(LANES) if VELOCITIES[q][0] == rows and VELOCITIES[q][1] == cols][0]


def outer(axis, sign):
    return heading(axis, sign) + [FRAC, CODE]


def roll(x, shift):
    return pltpu.roll(x, shift % x.shape[-1], x.ndim - 1)


def first_kernel(
    rows, cols, chunks, copies,
    pops, mass, flags, bubble, conversion,
    aux, low, high, left, right, tally,
):
    block = rows * cols
    masses, fractions, codes = [], [], []
    contributions = []
    for r in range(rows):
        at = pl.ds(r * cols, cols)
        density = pops[at, :]
        for q in range(1, LANES):
            density = density + pops[pl.ds(q * block + r * cols, cols), :]
        m = mass[at, :]
        flag = flags[at, :]
        fraction = jnp.clip(m / density, 0.0, 1.0)
        code = jnp.where(
            (flag == 1) & (conversion[at, :] == 1), FILLING, flag.astype(jnp.float32) + 1.0
        )
        aux[at, :] = m
        aux[pl.ds(block + r * cols, cols), :] = fraction
        aux[pl.ds(2 * block + r * cols, cols), :] = code
        aux[pl.ds(3 * block + r * cols, cols), :] = bubble[at, :].astype(jnp.float32)
        contributions.append(
            jnp.where(flag == 0, 1.0, jnp.where(flag == 1, 1.0 - fraction, 0.0))
        )

    def tile(channel, r):
        ref, base = (pops, channel) if channel < LANES else (aux, channel - LANES)
        return ref[pl.ds(base * block + r * cols, cols), :]

    def column(channel, c):
        ref, base = (pops, channel) if channel < LANES else (aux, channel - LANES)
        return ref[pl.ds(base * block + c, rows, stride=cols), :]

    for out, inner_row, outer_row, sign in ((low, 0, 1, -1), (high, rows - 1, rows - 2, 1)):
        for channel in range(CHANNELS):
            out[pl.ds(channel * cols, cols), :] = tile(channel, inner_row)
        for k, channel in enumerate(outer(0, sign)):
            out[pl.ds((CHANNELS + k) * cols, cols), :] = tile(channel, outer_row)
    tall = rows + 2
    for out, inner_col, outer_col, sign in ((left, 0, 1, -1), (right, cols - 1, cols - 2, 1)):
        for channel in range(CHANNELS):
            out[pl.ds(channel * tall + 1, rows), :] = column(channel, inner_col)
        for k, channel in enumerate(outer(1, sign)):
            out[pl.ds((CHANNELS + k) * tall + 1, rows), :] = column(channel, outer_col)

    ones = jnp.ones((8, 128), jnp.float32)
    lane_count = mass.shape[-1]

    def count(chunk):
        labels = lax.broadcasted_iota(jnp.int32, (128, lane_count), 0) + chunk * 128
        total = jnp.zeros((128, lane_count), jnp.float32)
        for r in range(rows):
            for c in range(cols):
                row = bubble[pl.ds(r * cols + c, 1), :]
                term = contributions[r][c : c + 1, :]
                total = total + jnp.where(labels == row, term, 0.0)
        return lax.dot_general(
            jnp.ones((8, lane_count), jnp.float32),
            total,
            (((1,), (1,)), ((), ())),
            precision=lax.Precision.HIGHEST,
            preferred_element_type=jnp.float32,
        )

    del ones
    for chunk in range(chunks):
        summed = count(chunk)
        for k in range(copies):
            tally[k, chunk] = summed


def second_kernel(rows, cols, low, high, left, right, left_out, right_out):
    tall = rows + 2
    for part, out, inner_col, outer_col, sign in (
        (left, left_out, 0, 1, -1),
        (right, right_out, cols - 1, cols - 2, 1),
    ):
        carried = (CHANNELS + len(outer(1, sign))) * tall
        out[pl.ds(0, carried), :] = part[pl.ds(0, carried), :]
        spare = carried
        for halo, row, towards in ((low, 0, 1), (high, tall - 1, -1)):
            out[pl.ds(row, CHANNELS, stride=tall), :] = halo[
                pl.ds(inner_col, CHANNELS, stride=cols), :
            ]
            for k, channel in enumerate(outer(1, sign)):
                out[pl.ds((CHANNELS + k) * tall + row, 1), :] = halo[
                    pl.ds(channel * cols + outer_col, 1), :
                ]
            beyond = outer(0, towards)
            out[pl.ds(spare, len(beyond)), :] = halo[
                pl.ds(CHANNELS * cols + inner_col, len(beyond), stride=cols), :
            ]
            spare += len(beyond)
            for channel in (heading_both(towards, sign), FRAC, CODE):
                k = beyond.index(channel)
                out[pl.ds(spare, 1), :] = halo[pl.ds((CHANNELS + k) * cols + outer_col, 1), :]
                spare += 1


def side_tiles(rows):
    tall = rows + 2
    used = (CHANNELS + 7) * tall + 2 * (7 + 3)
    return -(-used // 8) * 8


def third_kernel(
    rows, cols, chunks, copies, labels,
    pops, aux, low, high, left, right, tally, rest,
    relaxed_out, new_mass_out, gas_out,
    cells, near, sums, table, relaxed_stage, mass_stage, wet_sem, mass_sem,
):
    block = rows * cols
    tall = rows + 2
    high_rows = rows + 4
    wide = cols + 4
    total_rows = wide * high_rows

    for chunk in range(chunks):
        volume = tally[0, chunk]
        for k in range(1, copies):
            volume = volume + tally[k, chunk]
        here = min(128, labels - chunk * 128)
        gas = AMBIENT + rest[0:1, pl.ds(chunk * 128, here)] / jnp.maximum(volume[0:1, :here], 1.0)
        gas_out[0:1, pl.ds(chunk * 128, here)] = gas
        table[chunk, :, pl.ds(0, here)] = jnp.broadcast_to(gas, (8, here))

    for channel in range(CHANNELS):
        ref, base = (pops, channel) if channel < LANES else (aux, channel - LANES)
        for c in range(cols):
            cells[channel, pl.ds((c + 2) * high_rows + 2, rows), :] = ref[
                pl.ds(base * block + c, rows, stride=cols), :
            ]
    for halo, inner_row, outer_row, towards in (
        (low, 1, 0, 1),
        (high, high_rows - 2, high_rows - 1, -1),
    ):
        for channel in range(CHANNELS):
            cells[channel, pl.ds(2 * high_rows + inner_row, cols, stride=high_rows), :] = halo[
                pl.ds(channel * cols, cols), :
            ]
        for k, channel in enumerate(outer(0, towards)):
            cells[channel, pl.ds(2 * high_rows + outer_row, cols, stride=high_rows), :] = halo[
                pl.ds((CHANNELS + k) * cols, cols), :
            ]
    for halo, inner_col, outer_col, sign in (
        (left, 1, 0, 1),
        (right, wide - 2, wide - 1, -1),
    ):
        for channel in range(CHANNELS):
            cells[channel, pl.ds(inner_col * high_rows + 1, tall), :] = halo[
                pl.ds(channel * tall, tall), :
            ]
        for k, channel in enumerate(outer(1, sign)):
            cells[channel, pl.ds(outer_col * high_rows + 1, tall), :] = halo[
                pl.ds((CHANNELS + k) * tall, tall), :
            ]
        spare = (CHANNELS + 7) * tall
        for row, towards in ((0, 1), (high_rows - 1, -1)):
            for channel in outer(0, towards):
                cells[channel, pl.ds(inner_col * high_rows + row, 1), :] = halo[
                    pl.ds(spare, 1), :
                ]
                spare += 1
            for channel in (heading_both(towards, sign), FRAC, CODE):
                cells[channel, pl.ds(outer_col * high_rows + row, 1), :] = halo[
                    pl.ds(spare, 1), :
                ]
                spare += 1

    for begin in range(0, total_rows, 8):
        at = pl.ds(begin, min(8, total_rows - begin))
        code = cells[CODE, at, :]
        fraction = cells[FRAC, at, :]
        face = (code == FACE) | (code == FILLING)
        u = jnp.where(code == LIQUID, 1.0, jnp.where(face, 0.5 * fraction, 0.0))
        v = jnp.where(face, 0.5, 0.0)
        free = jnp.where(code == FACE, 1.0, 0.0)
        for depth in (-1, 0, 1):
            for k, value in enumerate((code, u, v)):
                near[k * 3 + depth + 1, at, :] = roll(value, depth) if depth else value
        ends = roll(free, 1) + roll(free, -1)
        near[9, at, :] = free
        near[10, at, :] = ends
        near[11, at, :] = free + ends

    def moments(tiles):
        density = tiles[0]
        for t in tiles[1:]:
            density = density + t
        flux = []
        for axis in range(3):
            plus = [tiles[q] for q in heading(axis, 1)]
            minus = [tiles[q] for q in heading(axis, -1)]
            j = plus[0] - minus[0]
            for a, b in zip(plus[1:], minus[1:]):
                j = j + (a - b)
            flux.append(j)
        inverse = 1.0 / density
        return density, [j * inverse for j in flux]

    def projection(velocity, q):
        terms = [
            velocity[axis] if VELOCITIES[q][axis] > 0 else -velocity[axis]
            for axis in range(3)
            if VELOCITIES[q][axis]
        ]
        out = terms[0]
        for t in terms[1:]:
            out = out + t
        return out

    updates, portions = [], []
    for c in range(-1, cols + 1):
        base = (c + 2) * high_rows + 1
        inside = 0 <= c < cols

        def source(array, q, cells=cells, base=base):
            begin = base - int(VELOCITIES[q][1]) * high_rows - int(VELOCITIES[q][0])
            return array[pl.ds(begin, tall), :]

        own = [cells[q, pl.ds(base, tall), :] for q in range(LANES)]
        mass = cells[MASS, pl.ds(base, tall), :]
        fraction = cells[FRAC, pl.ds(base, tall), :]
        code = cells[CODE, pl.ds(base, tall), :]
        bubble = cells[BUB, pl.ds(base, tall), :].astype(jnp.int32)
        gas = None
        for chunk in range(chunks):
            index = bubble - chunk * 128
            valid = (index >= 0) & (index < 128)
            found = jnp.take_along_axis(
                table[chunk, pl.ds(0, tall), :], jnp.where(valid, index, 0), axis=1
            )
            gas = found if gas is None else jnp.where(valid, found, gas)
        _, velocity = moments(own)
        still = 1.0 - 1.5 * (
            velocity[0] * velocity[0] + velocity[1] * velocity[1] + velocity[2] * velocity[2]
        )
        flow = None
        passed = [own[0]] + [None] * (LANES - 1)
        for first in range(1, LANES, 2):
            project = projection(velocity, first)
            pressed = gas * (2.0 * WEIGHTS[first]) * (still + 4.5 * project * project)
            for q in (first, first + 1):
                depth = int(VELOCITIES[q][2])
                moved = source(cells.at[q], q)
                if depth:
                    moved = roll(moved, depth)
                bounced = own[OPPOSITE[q]]
                kind = source(near.at[depth + 1], q)
                weight = source(near.at[3 + depth + 1], q) + source(near.at[6 + depth + 1], q) * fraction
                term = weight * (moved - bounced)
                flow = term if flow is None else flow + term
                passed[q] = jnp.where(
                    kind == GAS, pressed - bounced, jnp.where(kind == WALL, bounced, moved)
                )
        targets = near[10, pl.ds(base, tall), :]
        for dr in (-1, 0, 1):
            for dc in (-1, 0, 1):
                if dr or dc:
                    plane = 9 if dr and dc else 11
                    targets = targets + near[plane, pl.ds(base + dc * high_rows + dr, tall), :]
        filling = code == FILLING
        if inside:
            density, moved_velocity = moments(passed)
        else:
            density = passed[0]
            for t in passed[1:]:
                density = density + t
        taken = mass + flow
        portion = jnp.where(filling, (taken - density) / jnp.maximum(targets, 1.0), 0.0)
        portions.append(portion)
        if inside:
            updates.append(
                jnp.where(
                    code == FACE,
                    taken,
                    jnp.where((code == LIQUID) | filling, density, mass),
                )
            )
            dry = code == GAS
            still = 1.0 - 1.5 * (
                moved_velocity[0] * moved_velocity[0]
                + moved_velocity[1] * moved_velocity[1]
                + moved_velocity[2] * moved_velocity[2]
            )
            scaled = RELAX * density

            def put(q, value, own=own, c=c, dry=dry):
                relaxed_stage[pl.ds(q * tall * cols + c, tall, stride=cols), :] = jnp.where(
                    dry, own[q], value
                )

            put(0, (1.0 - RELAX) * passed[0] + (scaled * WEIGHTS[0]) * still)
            for first in range(1, LANES, 2):
                project = projection(moved_velocity, first)
                even = still + 4.5 * project * project
                odd = 3.0 * project
                share = scaled * WEIGHTS[first]
                put(first, (1.0 - RELAX) * passed[first] + share * (even + odd))
                put(first + 1, (1.0 - RELAX) * passed[first + 1] + share * (even - odd))

    relaxed_copies = [
        pltpu.make_async_copy(
            relaxed_stage.at[pl.ds((q * tall + 1) * cols, block), :],
            relaxed_out.at[pl.ds(q * block, block), :],
            wet_sem.at[q],
        )
        for q in range(LANES)
    ]
    for copy in relaxed_copies:
        copy.start()

    ends = [roll(p, 1) + roll(p, -1) for p in portions]
    full = [p + e for p, e in zip(portions, ends)]
    for c in range(cols):
        beside = ends[c + 1] + full[c] + full[c + 2]
        stacked = full[c + 1] + portions[c] + portions[c + 2]
        sums[pl.ds(8, tall), :] = stacked
        gained = beside + sums[pl.ds(7, tall), :] + sums[pl.ds(9, tall), :]
        code = cells[CODE, pl.ds((c + 2) * high_rows + 1, tall), :]
        mass_stage[pl.ds(c, tall, stride=cols), :] = jnp.where(
            code == FACE, updates[c] + gained, updates[c]
        )
    mass_copy = pltpu.make_async_copy(
        mass_stage.at[pl.ds(cols, block), :], new_mass_out, mass_sem
    )
    mass_copy.start()
    for copy in relaxed_copies:
        copy.wait()
    mass_copy.wait()


def shards(gx_size, gy_size, populations, cell_mass, cell_flags, bubble, conversion, rest_volume):
    rows, cols, depth = populations.shape[1:]
    labels = rest_volume.shape[0]
    block = rows * cols
    tall = rows + 2
    devices = gx_size * gy_size
    chunks = -(-labels // 128)
    direct = devices * chunks <= 64
    copies = devices if direct else 1
    f32 = jnp.float32
    vmem = pl.BlockSpec(memory_space=pltpu.VMEM)

    pops = populations.reshape(LANES * block, depth)
    flat = [a.reshape(block, depth) for a in (cell_mass, cell_flags, bubble, conversion)]
    end_rows = (CHANNELS + 7) * cols
    side_rows = side_tiles(rows)

    aux, low, high, left, right, tally = pl.pallas_call(
        functools.partial(first_kernel, rows, cols, chunks, copies),
        out_shape=[
            jax.ShapeDtypeStruct((4 * block, depth), f32),
            jax.ShapeDtypeStruct((end_rows, depth), f32),
            jax.ShapeDtypeStruct((end_rows, depth), f32),
            jax.ShapeDtypeStruct((side_rows, depth), f32),
            jax.ShapeDtypeStruct((side_rows, depth), f32),
            jax.ShapeDtypeStruct((copies, chunks, 8, 128), f32),
        ],
        in_specs=[vmem] * 5,
        out_specs=[vmem] * 6,
        cost_estimate=pl.CostEstimate(flops=2000000, bytes_accessed=2000000, transcendentals=0),
        name="pack",
    )(pops, *flat)

    def shifted(x, axis, size, up):
        pairs = [(i, i + 1) if up else (i + 1, i) for i in range(size - 1)]
        return lax.ppermute(x, axis, pairs)

    from_below = shifted(high, "gx", gx_size, True)
    from_above = shifted(low, "gx", gx_size, False)
    if direct:
        tallies = lax.all_to_all(
            tally.reshape(devices, chunks * 8, 128), ("gx", "gy"), 0, 0
        ).reshape(devices, chunks, 8, 128)
    else:
        tallies = lax.psum(tally[0, :, 0], ("gx", "gy"))
        tallies = jnp.broadcast_to(tallies[None, :, None, :], (1, chunks, 8, 128))

    left, right = pl.pallas_call(
        functools.partial(second_kernel, rows, cols),
        out_shape=[jax.ShapeDtypeStruct((side_rows, depth), f32)] * 2,
        in_specs=[vmem] * 4,
        out_specs=[vmem] * 2,
        name="relay",
    )(from_below, from_above, left, right)
    from_left = shifted(right, "gy", gy_size, True)
    from_right = shifted(left, "gy", gy_size, False)

    relaxed, new_mass, gas = pl.pallas_call(
        functools.partial(third_kernel, rows, cols, chunks, copies, labels),
        out_shape=[
            jax.ShapeDtypeStruct((LANES * block, depth), f32),
            jax.ShapeDtypeStruct((block, depth), f32),
            jax.ShapeDtypeStruct((1, labels), f32),
        ],
        in_specs=[vmem] * 8,
        out_specs=[
            pl.BlockSpec(memory_space=pl.ANY),
            pl.BlockSpec(memory_space=pl.ANY),
            vmem,
        ],
        scratch_shapes=[
            pltpu.VMEM((CHANNELS, (cols + 4) * (rows + 4), depth), f32),
            pltpu.VMEM((12, (cols + 4) * (rows + 4), depth), f32),
            pltpu.VMEM((24, depth), f32),
            pltpu.VMEM((chunks, 8, 128), f32),
            pltpu.VMEM((LANES * tall * cols, depth), f32),
            pltpu.VMEM((tall * cols, depth), f32),
            pltpu.SemaphoreType.DMA((LANES,)),
            pltpu.SemaphoreType.DMA,
        ],
        cost_estimate=pl.CostEstimate(flops=5000000, bytes_accessed=3000000, transcendentals=0),
        name="settle",
    )(pops, aux, from_below, from_above, from_left, from_right, tallies, rest_volume.reshape(1, labels))
    return (
        relaxed.reshape(LANES, rows, cols, depth),
        new_mass.reshape(rows, cols, depth),
        gas.reshape(labels),
    )


def solution(mesh):
    placed = (
        P(None, "gx", "gy", None),
        P("gx", "gy", None),
        P("gx", "gy", None),
        P("gx", "gy", None),
        P("gx", "gy", None),
        P(),
    )
    return jax.shard_map(
        functools.partial(shards, mesh.shape["gx"], mesh.shape["gy"]),
        mesh=mesh,
        in_specs=placed,
        out_specs=(P(None, "gx", "gy", None), P("gx", "gy", None), P()),
        check_vma=False,
    )
```

```python
import functools

import jax
import jax.numpy as jnp
import numpy as np
from jax import lax
from jax.experimental import pallas as pl
from jax.experimental.pallas import tpu as pltpu
from jax.sharding import PartitionSpec as P

VELOCITIES = np.array(
    [
        [0, 0, 0],
        [1, 0, 0],
        [-1, 0, 0],
        [0, 1, 0],
        [0, -1, 0],
        [0, 0, 1],
        [0, 0, -1],
        [1, 1, 0],
        [-1, -1, 0],
        [1, -1, 0],
        [-1, 1, 0],
        [1, 0, 1],
        [-1, 0, -1],
        [1, 0, -1],
        [-1, 0, 1],
        [0, 1, 1],
        [0, -1, -1],
        [0, 1, -1],
        [0, -1, 1],
    ]
)
OPPOSITE = [0, 2, 1, 4, 3, 6, 5, 8, 7, 10, 9, 12, 11, 14, 13, 16, 15, 18, 17]
WEIGHTS = [1.0 / 3.0] + [1.0 / 18.0] * 6 + [1.0 / 36.0] * 12
RELAX = 1.0 / 0.6
AMBIENT = 2.0
LANES = 19
MASS, FRAC, CODE, BUB = 19, 20, 21, 22
CHANNELS = 23
WALL, GAS, FACE, LIQUID, FILLING = 0.0, 1.0, 2.0, 3.0, 5.0


def heading(axis, sign):
    return [q for q in range(LANES) if VELOCITIES[q][axis] == sign]


def heading_both(rows, cols):
    return [q for q in range(LANES) if VELOCITIES[q][0] == rows and VELOCITIES[q][1] == cols][0]


def outer(axis, sign):
    return heading(axis, sign) + [FRAC, CODE]


def roll(x, shift):
    return pltpu.roll(x, shift % x.shape[-1], x.ndim - 1)


def by_parity(axis, use, even, odd):
    odd_device = lax.rem(lax.axis_index(axis), 2) == 1

    @pl.when(odd_device)
    def _():
        use(even, odd)

    @pl.when(jnp.logical_not(odd_device))
    def _():
        use(odd, even)


def paired(size, odd):
    pairs = []
    for i in range(1 if odd else 0, size - 1, 2):
        pairs += [(i, i + 1), (i + 1, i)]
    return pairs


def first_kernel(
    rows, cols, chunks, copies,
    pops_in, mass_in, flags_in, bubble_in, conversion_in, rest,
    aux, across_even, across_odd, beside_even, beside_odd, rest_table, tally,
    pops, mass, flags, bubble, conversion, sems,
):
    block = rows * cols
    copies_in = [
        pltpu.make_async_copy(a, b, sems.at[k])
        for k, (a, b) in enumerate(
            (
                (pops_in, pops),
                (mass_in, mass),
                (flags_in, flags),
                (bubble_in, bubble),
                (conversion_in, conversion),
            )
        )
    ]
    for copy in copies_in:
        copy.start()
    labels_all = rest.shape[-1]
    for chunk in range(chunks):
        here = min(128, labels_all - chunk * 128)
        rest_table[chunk, :, pl.ds(0, here)] = jnp.broadcast_to(
            rest[0:1, pl.ds(chunk * 128, here)], (8, here)
        )
    for copy in copies_in:
        copy.wait()
    masses, fractions, codes = [], [], []
    contributions = []
    for r in range(rows):
        at = pl.ds(r * cols, cols)
        density = pops[at, :]
        for q in range(1, LANES):
            density = density + pops[pl.ds(q * block + r * cols, cols), :]
        m = mass[at, :]
        flag = flags[at, :]
        fraction = jnp.clip(m / density, 0.0, 1.0)
        code = jnp.where(
            (flag == 1) & (conversion[at, :] == 1), FILLING, flag.astype(jnp.float32) + 1.0
        )
        aux[at, :] = m
        aux[pl.ds(block + r * cols, cols), :] = fraction
        aux[pl.ds(2 * block + r * cols, cols), :] = code
        aux[pl.ds(3 * block + r * cols, cols), :] = bubble[at, :].astype(jnp.float32)
        contributions.append(
            jnp.where(flag == 0, 1.0, jnp.where(flag == 1, 1.0 - fraction, 0.0))
        )

    def tile(channel, r):
        ref, base = (pops, channel) if channel < LANES else (aux, channel - LANES)
        return ref[pl.ds(base * block + r * cols, cols), :]

    def column(channel, c):
        ref, base = (pops, channel) if channel < LANES else (aux, channel - LANES)
        return ref[pl.ds(base * block + c, rows, stride=cols), :]

    tall = rows + 2

    def send_rows(out, inner_row, outer_row, sign):
        for channel in range(CHANNELS):
            out[pl.ds(channel * cols, cols), :] = tile(channel, inner_row)
        for k, channel in enumerate(outer(0, sign)):
            out[pl.ds((CHANNELS + k) * cols, cols), :] = tile(channel, outer_row)

    def send_cols(out, inner_col, outer_col, sign):
        for channel in range(CHANNELS):
            out[pl.ds(channel * tall + 1, rows), :] = column(channel, inner_col)
        for k, channel in enumerate(outer(1, sign)):
            out[pl.ds((CHANNELS + k) * tall + 1, rows), :] = column(channel, outer_col)

    def low_high(low, high):
        send_rows(low, 0, 1, -1)
        send_rows(high, rows - 1, rows - 2, 1)

    def left_right(left, right):
        send_cols(left, 0, 1, -1)
        send_cols(right, cols - 1, cols - 2, 1)

    by_parity("gx", low_high, across_even, across_odd)
    by_parity("gy", left_right, beside_even, beside_odd)

    lane_count = mass.shape[-1]

    def count(chunk):
        labels = lax.broadcasted_iota(jnp.int32, (128, lane_count), 0) + chunk * 128
        total = jnp.zeros((128, lane_count), jnp.float32)
        for r in range(rows):
            for c in range(cols):
                row = bubble[pl.ds(r * cols + c, 1), :]
                term = contributions[r][c : c + 1, :]
                total = total + jnp.where(labels == row, term, 0.0)
        return lax.dot_general(
            jnp.ones((8, lane_count), jnp.float32),
            total,
            (((1,), (1,)), ((), ())),
            precision=lax.Precision.HIGHEST,
            preferred_element_type=jnp.float32,
        )

    for chunk in range(chunks):
        summed = count(chunk)
        for k in range(copies):
            tally[k, chunk] = summed


def second_kernel(rows, cols, across_even, across_odd, beside_even, beside_odd, even_out, odd_out):
    def with_rows(low, high):
        def with_cols(left_pair, right_pair):
            relay(rows, cols, low, high, *left_pair, *right_pair)

        by_parity("gy", with_cols, (beside_even, even_out), (beside_odd, odd_out))

    by_parity("gx", with_rows, across_even, across_odd)


def relay(rows, cols, low, high, left, left_out, right, right_out):
    tall = rows + 2
    for part, out, inner_col, outer_col, sign in (
        (left, left_out, 0, 1, -1),
        (right, right_out, cols - 1, cols - 2, 1),
    ):
        carried = (CHANNELS + len(outer(1, sign))) * tall
        out[pl.ds(0, carried), :] = part[pl.ds(0, carried), :]
        spare = carried
        for halo, row, towards in ((low, 0, 1), (high, tall - 1, -1)):
            out[pl.ds(row, CHANNELS, stride=tall), :] = halo[
                pl.ds(inner_col, CHANNELS, stride=cols), :
            ]
            for k, channel in enumerate(outer(1, sign)):
                out[pl.ds((CHANNELS + k) * tall + row, 1), :] = halo[
                    pl.ds(channel * cols + outer_col, 1), :
                ]
            beyond = outer(0, towards)
            out[pl.ds(spare, len(beyond)), :] = halo[
                pl.ds(CHANNELS * cols + inner_col, len(beyond), stride=cols), :
            ]
            spare += len(beyond)
            for channel in (heading_both(towards, sign), FRAC, CODE):
                k = beyond.index(channel)
                out[pl.ds(spare, 1), :] = halo[pl.ds((CHANNELS + k) * cols + outer_col, 1), :]
                spare += 1


def side_tiles(rows):
    tall = rows + 2
    used = (CHANNELS + 7) * tall + 2 * (7 + 3)
    return -(-used // 8) * 8


def third_kernel(
    rows, cols, chunks, copies, labels,
    pops, aux, across_even, across_odd, beside_even, beside_odd, tally, rest,
    relaxed_out, new_mass_out, gas_out,
    cells, near, sums, table, relaxed_stage, mass_stage, wet_sem, mass_sem,
):
    block = rows * cols
    tall = rows + 2
    high_rows = rows + 4
    wide = cols + 4
    total_rows = wide * high_rows

    for chunk in range(chunks):
        volume = tally[0, chunk]
        for k in range(1, copies):
            volume = volume + tally[k, chunk]
        here = min(128, labels - chunk * 128)
        gas = AMBIENT + rest[chunk] / jnp.maximum(volume, 1.0)
        gas_out[0:1, pl.ds(chunk * 128, here)] = gas[0:1, :here]
        table[chunk] = gas

    for channel in range(CHANNELS):
        ref, base = (pops, channel) if channel < LANES else (aux, channel - LANES)
        for c in range(cols):
            cells[channel, pl.ds((c + 2) * high_rows + 2, rows), :] = ref[
                pl.ds(base * block + c, rows, stride=cols), :
            ]
    def fill_rows(low, high):
        for halo, inner_row, outer_row, towards in (
            (low, 1, 0, 1),
            (high, high_rows - 2, high_rows - 1, -1),
        ):
            for channel in range(CHANNELS):
                cells[channel, pl.ds(2 * high_rows + inner_row, cols, stride=high_rows), :] = halo[
                    pl.ds(channel * cols, cols), :
                ]
            for k, channel in enumerate(outer(0, towards)):
                cells[channel, pl.ds(2 * high_rows + outer_row, cols, stride=high_rows), :] = halo[
                    pl.ds((CHANNELS + k) * cols, cols), :
                ]

    def fill_cols(left, right):
        for halo, inner_col, outer_col, sign in (
            (left, 1, 0, 1),
            (right, wide - 2, wide - 1, -1),
        ):
            for channel in range(CHANNELS):
                cells[channel, pl.ds(inner_col * high_rows + 1, tall), :] = halo[
                    pl.ds(channel * tall, tall), :
                ]
            for k, channel in enumerate(outer(1, sign)):
                cells[channel, pl.ds(outer_col * high_rows + 1, tall), :] = halo[
                    pl.ds((CHANNELS + k) * tall, tall), :
                ]
            spare = (CHANNELS + 7) * tall
            for row, towards in ((0, 1), (high_rows - 1, -1)):
                for channel in outer(0, towards):
                    cells[channel, pl.ds(inner_col * high_rows + row, 1), :] = halo[
                        pl.ds(spare, 1), :
                    ]
                    spare += 1
                for channel in (heading_both(towards, sign), FRAC, CODE):
                    cells[channel, pl.ds(outer_col * high_rows + row, 1), :] = halo[
                        pl.ds(spare, 1), :
                    ]
                    spare += 1

    by_parity("gx", fill_rows, across_even, across_odd)
    by_parity("gy", fill_cols, beside_even, beside_odd)

    for begin in range(0, total_rows, 8):
        at = pl.ds(begin, min(8, total_rows - begin))
        code = cells[CODE, at, :]
        fraction = cells[FRAC, at, :]
        face = (code == FACE) | (code == FILLING)
        u = jnp.where(code == LIQUID, 1.0, jnp.where(face, 0.5 * fraction, 0.0))
        v = jnp.where(face, 0.5, 0.0)
        free = jnp.where(code == FACE, 1.0, 0.0)
        for depth in (-1, 0, 1):
            for k, value in enumerate((code, u, v)):
                near[k * 3 + depth + 1, at, :] = roll(value, depth) if depth else value
        ends = roll(free, 1) + roll(free, -1)
        near[9, at, :] = free
        near[10, at, :] = ends
        near[11, at, :] = free + ends

    def moments(tiles):
        density = tiles[0]
        for t in tiles[1:]:
            density = density + t
        flux = []
        for axis in range(3):
            plus = [tiles[q] for q in heading(axis, 1)]
            minus = [tiles[q] for q in heading(axis, -1)]
            j = plus[0] - minus[0]
            for a, b in zip(plus[1:], minus[1:]):
                j = j + (a - b)
            flux.append(j)
        inverse = 1.0 / density
        return density, [j * inverse for j in flux]

    def projection(velocity, q):
        terms = [
            velocity[axis] if VELOCITIES[q][axis] > 0 else -velocity[axis]
            for axis in range(3)
            if VELOCITIES[q][axis]
        ]
        out = terms[0]
        for t in terms[1:]:
            out = out + t
        return out

    updates, portions = [], []
    for c in range(-1, cols + 1):
        base = (c + 2) * high_rows + 1
        inside = 0 <= c < cols

        def source(array, q, cells=cells, base=base):
            begin = base - int(VELOCITIES[q][1]) * high_rows - int(VELOCITIES[q][0])
            return array[pl.ds(begin, tall), :]

        own = [cells[q, pl.ds(base, tall), :] for q in range(LANES)]
        mass = cells[MASS, pl.ds(base, tall), :]
        fraction = cells[FRAC, pl.ds(base, tall), :]
        code = cells[CODE, pl.ds(base, tall), :]
        bubble = cells[BUB, pl.ds(base, tall), :].astype(jnp.int32)
        gas = None
        for chunk in range(chunks):
            index = bubble - chunk * 128
            valid = (index >= 0) & (index < 128)
            found = jnp.take_along_axis(
                table[chunk, pl.ds(0, tall), :], jnp.where(valid, index, 0), axis=1
            )
            gas = found if gas is None else jnp.where(valid, found, gas)
        _, velocity = moments(own)
        still = 1.0 - 1.5 * (
            velocity[0] * velocity[0] + velocity[1] * velocity[1] + velocity[2] * velocity[2]
        )
        flow = None
        passed = [own[0]] + [None] * (LANES - 1)
        for first in range(1, LANES, 2):
            project = projection(velocity, first)
            pressed = gas * (2.0 * WEIGHTS[first]) * (still + 4.5 * project * project)
            for q in (first, first + 1):
                depth = int(VELOCITIES[q][2])
                moved = source(cells.at[q], q)
                if depth:
                    moved = roll(moved, depth)
                bounced = own[OPPOSITE[q]]
                kind = source(near.at[depth + 1], q)
                weight = source(near.at[3 + depth + 1], q) + source(near.at[6 + depth + 1], q) * fraction
                term = weight * (moved - bounced)
                flow = term if flow is None else flow + term
                passed[q] = jnp.where(
                    kind == GAS, pressed - bounced, jnp.where(kind == WALL, bounced, moved)
                )
        targets = near[10, pl.ds(base, tall), :]
        for dr in (-1, 0, 1):
            for dc in (-1, 0, 1):
                if dr or dc:
                    plane = 9 if dr and dc else 11
                    targets = targets + near[plane, pl.ds(base + dc * high_rows + dr, tall), :]
        filling = code == FILLING
        if inside:
            density, moved_velocity = moments(passed)
        else:
            density = passed[0]
            for t in passed[1:]:
                density = density + t
        taken = mass + flow
        portion = jnp.where(filling, (taken - density) / jnp.maximum(targets, 1.0), 0.0)
        portions.append(portion)
        if inside:
            updates.append(
                jnp.where(
                    code == FACE,
                    taken,
                    jnp.where((code == LIQUID) | filling, density, mass),
                )
            )
            dry = code == GAS
            still = 1.0 - 1.5 * (
                moved_velocity[0] * moved_velocity[0]
                + moved_velocity[1] * moved_velocity[1]
                + moved_velocity[2] * moved_velocity[2]
            )
            scaled = RELAX * density

            def put(q, value, own=own, c=c, dry=dry):
                relaxed_stage[pl.ds(q * tall * cols + c, tall, stride=cols), :] = jnp.where(
                    dry, own[q], value
                )

            put(0, (1.0 - RELAX) * passed[0] + (scaled * WEIGHTS[0]) * still)
            for first in range(1, LANES, 2):
                project = projection(moved_velocity, first)
                even = still + 4.5 * project * project
                odd = 3.0 * project
                share = scaled * WEIGHTS[first]
                put(first, (1.0 - RELAX) * passed[first] + share * (even + odd))
                put(first + 1, (1.0 - RELAX) * passed[first + 1] + share * (even - odd))

    relaxed_copies = [
        pltpu.make_async_copy(
            relaxed_stage.at[pl.ds((q * tall + 1) * cols, block), :],
            relaxed_out.at[pl.ds(q * block, block), :],
            wet_sem.at[q],
        )
        for q in range(LANES)
    ]
    for copy in relaxed_copies:
        copy.start()

    ends = [roll(p, 1) + roll(p, -1) for p in portions]
    full = [p + e for p, e in zip(portions, ends)]
    for c in range(cols):
        beside = ends[c + 1] + full[c] + full[c + 2]
        stacked = full[c + 1] + portions[c] + portions[c + 2]
        sums[pl.ds(8, tall), :] = stacked
        gained = beside + sums[pl.ds(7, tall), :] + sums[pl.ds(9, tall), :]
        code = cells[CODE, pl.ds((c + 2) * high_rows + 1, tall), :]
        mass_stage[pl.ds(c, tall, stride=cols), :] = jnp.where(
            code == FACE, updates[c] + gained, updates[c]
        )
    mass_copy = pltpu.make_async_copy(
        mass_stage.at[pl.ds(cols, block), :], new_mass_out, mass_sem
    )
    mass_copy.start()
    for copy in relaxed_copies:
        copy.wait()
    mass_copy.wait()


def shards(gx_size, gy_size, populations, cell_mass, cell_flags, bubble, conversion, rest_volume):
    rows, cols, depth = populations.shape[1:]
    labels = rest_volume.shape[0]
    block = rows * cols
    tall = rows + 2
    devices = gx_size * gy_size
    chunks = -(-labels // 128)
    direct = devices * chunks <= 64
    copies = devices if direct else 1
    f32 = jnp.float32
    vmem = pl.BlockSpec(memory_space=pltpu.VMEM)
    hbm = pl.BlockSpec(memory_space=pltpu.HBM)

    pops = populations.reshape(LANES * block, depth)
    flat = [a.reshape(block, depth) for a in (cell_mass, cell_flags, bubble, conversion)]
    end_rows = (CHANNELS + 7) * cols
    side_rows = side_tiles(rows)

    aux, across_even, across_odd, beside_even, beside_odd, rest, tally = pl.pallas_call(
        functools.partial(first_kernel, rows, cols, chunks, copies),
        out_shape=[
            jax.ShapeDtypeStruct((4 * block, depth), f32),
            jax.ShapeDtypeStruct((end_rows, depth), f32),
            jax.ShapeDtypeStruct((end_rows, depth), f32),
            jax.ShapeDtypeStruct((side_rows, depth), f32),
            jax.ShapeDtypeStruct((side_rows, depth), f32),
            jax.ShapeDtypeStruct((chunks, 8, 128), f32),
            jax.ShapeDtypeStruct((copies, chunks, 8, 128), f32),
        ],
        in_specs=[hbm] * 5 + [vmem],
        out_specs=[vmem] * 7,
        scratch_shapes=[
            pltpu.VMEM((LANES * block, depth), f32),
            pltpu.VMEM((block, depth), f32),
            pltpu.VMEM((block, depth), jnp.int32),
            pltpu.VMEM((block, depth), jnp.int32),
            pltpu.VMEM((block, depth), jnp.int32),
            pltpu.SemaphoreType.DMA((5,)),
        ],
        cost_estimate=pl.CostEstimate(flops=2000000, bytes_accessed=2000000, transcendentals=0),
        compiler_params=pltpu.CompilerParams(vmem_limit_bytes=67043328),
        name="pack",
    )(pops, *flat, rest_volume.reshape(1, labels))

    def swapped(x, axis, size, odd):
        return lax.ppermute(x, axis, paired(size, odd))

    across_odd = swapped(across_odd, "gx", gx_size, True)
    across_even = swapped(across_even, "gx", gx_size, False)
    if direct:
        tallies = lax.all_to_all(
            tally.reshape(devices, chunks * 8, 128), ("gx", "gy"), 0, 0
        ).reshape(devices, chunks, 8, 128)
    else:
        tallies = lax.psum(tally[0, :, 0], ("gx", "gy"))
        tallies = jnp.broadcast_to(tallies[None, :, None, :], (1, chunks, 8, 128))

    beside_even, beside_odd = pl.pallas_call(
        functools.partial(second_kernel, rows, cols),
        out_shape=[jax.ShapeDtypeStruct((side_rows, depth), f32)] * 2,
        in_specs=[vmem] * 4,
        out_specs=[vmem] * 2,
        compiler_params=pltpu.CompilerParams(vmem_limit_bytes=4 << 20),
        name="relay",
    )(across_even, across_odd, beside_even, beside_odd)
    beside_odd = swapped(beside_odd, "gy", gy_size, True)
    beside_even = swapped(beside_even, "gy", gy_size, False)

    relaxed, new_mass, gas = pl.pallas_call(
        functools.partial(third_kernel, rows, cols, chunks, copies, labels),
        out_shape=[
            jax.ShapeDtypeStruct((LANES * block, depth), f32),
            jax.ShapeDtypeStruct((block, depth), f32),
            jax.ShapeDtypeStruct((1, labels), f32),
        ],
        in_specs=[vmem] * 8,
        out_specs=[
            pl.BlockSpec(memory_space=pl.ANY),
            pl.BlockSpec(memory_space=pl.ANY),
            vmem,
        ],
        scratch_shapes=[
            pltpu.VMEM((CHANNELS, (cols + 4) * (rows + 4), depth), f32),
            pltpu.VMEM((12, (cols + 4) * (rows + 4), depth), f32),
            pltpu.VMEM((24, depth), f32),
            pltpu.VMEM((chunks, 8, 128), f32),
            pltpu.VMEM((LANES * tall * cols, depth), f32),
            pltpu.VMEM((tall * cols, depth), f32),
            pltpu.SemaphoreType.DMA((LANES,)),
            pltpu.SemaphoreType.DMA,
        ],
        cost_estimate=pl.CostEstimate(flops=5000000, bytes_accessed=3000000, transcendentals=0),
        compiler_params=pltpu.CompilerParams(vmem_limit_bytes=12 << 20),
        name="settle",
    )(pops, aux, across_even, across_odd, beside_even, beside_odd, tallies, rest)
    return (
        relaxed.reshape(LANES, rows, cols, depth),
        new_mass.reshape(rows, cols, depth),
        gas.reshape(labels),
    )


def solution(mesh):
    placed = (
        P(None, "gx", "gy", None),
        P("gx", "gy", None),
        P("gx", "gy", None),
        P("gx", "gy", None),
        P("gx", "gy", None),
        P(),
    )
    return jax.shard_map(
        functools.partial(shards, mesh.shape["gx"], mesh.shape["gy"]),
        mesh=mesh,
        in_specs=placed,
        out_specs=(P(None, "gx", "gy", None), P("gx", "gy", None), P()),
        check_vma=False,
    )
```

```python
import functools

import jax
import jax.numpy as jnp
import numpy as np
from jax import lax
from jax.experimental import pallas as pl
from jax.experimental.pallas import tpu as pltpu
from jax.sharding import PartitionSpec as P


VELOCITIES = np.array(
    [
        [0, 0, 0],
        [1, 0, 0],
        [-1, 0, 0],
        [0, 1, 0],
        [0, -1, 0],
        [0, 0, 1],
        [0, 0, -1],
        [1, 1, 0],
        [-1, -1, 0],
        [1, -1, 0],
        [-1, 1, 0],
        [1, 0, 1],
        [-1, 0, -1],
        [1, 0, -1],
        [-1, 0, 1],
        [0, 1, 1],
        [0, -1, -1],
        [0, 1, -1],
        [0, -1, 1],
    ]
)
OPPOSITE = [0, 2, 1, 4, 3, 6, 5, 8, 7, 10, 9, 12, 11, 14, 13, 16, 15, 18, 17]
WEIGHTS = [1.0 / 3.0] + [1.0 / 18.0] * 6 + [1.0 / 36.0] * 12
RELAX = 1.0 / 0.6
AMBIENT = 2.0
HOLD = 2000000000
LANES = 19
MASS, FRAC, CODE, BUB = 19, 20, 21, 22
CHANNELS = 23
WALL, GAS, FACE, LIQUID, FILLING = 0.0, 1.0, 2.0, 3.0, 5.0


def heading(axis, sign):
    return [q for q in range(LANES) if VELOCITIES[q][axis] == sign]


def heading_both(rows, cols):
    return [q for q in range(LANES) if VELOCITIES[q][0] == rows and VELOCITIES[q][1] == cols][0]


def outer(axis, sign):
    return heading(axis, sign) + [FRAC, CODE]


def roll(x, shift):
    return pltpu.roll(x, shift % x.shape[-1], x.ndim - 1)


def by_parity(axis, use, even, odd):
    odd_device = lax.rem(lax.axis_index(axis), 2) == 1

    @pl.when(odd_device)
    def _():
        use(even, odd)

    @pl.when(jnp.logical_not(odd_device))
    def _():
        use(odd, even)


def paired(size, odd):
    pairs = []
    for i in range(1 if odd else 0, size - 1, 2):
        pairs += [(i, i + 1), (i + 1, i)]
    return pairs


def first_kernel(
    rows, cols, chunks, copies,
    pops_in, mass_in, flags_in, bubble_in, conversion_in, rest,
    across_even_out, across_odd_out, rest_out, tally_out,
    aux, pops, mass, flags, bubble, conversion, rest_in, sems,
    across_even, across_odd, rest_table, tally, out_sems,
):
    block = rows * cols
    copies_in = [
        pltpu.make_async_copy(a, b, sems.at[k])
        for k, (a, b) in enumerate(
            (
                (pops_in, pops),
                (mass_in, mass),
                (flags_in, flags),
                (bubble_in, bubble),
                (conversion_in, conversion),
                (rest, rest_in),
            )
        )
    ]
    for copy in copies_in:
        copy.start()
    for copy in copies_in:
        copy.wait()
    sent = []

    def send(k, staged, out):
        copy = pltpu.make_async_copy(staged, out, out_sems.at[k])
        copy.start()
        sent.append(copy)

    labels_all = rest.shape[-1]
    for chunk in range(chunks):
        here = min(128, labels_all - chunk * 128)
        rest_table[chunk, :, pl.ds(0, here)] = jnp.broadcast_to(
            rest_in[0:1, pl.ds(chunk * 128, here)], (8, here)
        )
    send(2, rest_table, rest_out)
    contributions = []
    for r in range(rows):
        at = pl.ds(r * cols, cols)
        density = pops[at, :]
        for q in range(1, LANES):
            density = density + pops[pl.ds(q * block + r * cols, cols), :]
        m = mass[at, :]
        flag = flags[at, :]
        fraction = jnp.clip(m / density, 0.0, 1.0)
        code = jnp.where(
            (flag == 1) & (conversion[at, :] == 1), FILLING, flag.astype(jnp.float32) + 1.0
        )
        aux[at, :] = m
        aux[pl.ds(block + r * cols, cols), :] = fraction
        aux[pl.ds(2 * block + r * cols, cols), :] = code
        aux[pl.ds(3 * block + r * cols, cols), :] = bubble[at, :].astype(jnp.float32)
        contributions.append(
            jnp.where(flag == 0, 1.0, jnp.where(flag == 1, 1.0 - fraction, 0.0))
        )

    def tile(channel, r):
        ref, base = (pops, channel) if channel < LANES else (aux, channel - LANES)
        return ref[pl.ds(base * block + r * cols, cols), :]

    def send_rows(out, inner_row, outer_row, sign):
        for channel in range(CHANNELS):
            out[pl.ds(channel * cols, cols), :] = tile(channel, inner_row)
        for k, channel in enumerate(outer(0, sign)):
            out[pl.ds((CHANNELS + k) * cols, cols), :] = tile(channel, outer_row)

    def low_high(low, high):
        send_rows(low, 0, 1, -1)
        send_rows(high, rows - 1, rows - 2, 1)

    by_parity("gx", low_high, across_even, across_odd)
    send(0, across_even, across_even_out)
    send(1, across_odd, across_odd_out)

    lane_count = mass.shape[-1]

    def count(chunk):
        labels = lax.broadcasted_iota(jnp.int32, (128, lane_count), 0) + chunk * 128
        total = jnp.zeros((128, lane_count), jnp.float32)
        for r in range(rows):
            for c in range(cols):
                row = bubble[pl.ds(r * cols + c, 1), :]
                term = contributions[r][c : c + 1, :]
                total = total + jnp.where(labels == row, term, 0.0)
        return lax.dot_general(
            jnp.ones((8, lane_count), jnp.float32),
            total,
            (((1,), (1,)), ((), ())),
            precision=lax.Precision.HIGHEST,
            preferred_element_type=jnp.float32,
        )

    for chunk in range(chunks):
        summed = count(chunk)
        for k in range(copies):
            tally[k, chunk] = summed
    send(3, tally, tally_out)
    for copy in sent:
        copy.wait()


def column_cells(rows, cols, c, pops, mass, flags, bubble, conversion):
    at = pl.ds(c, rows, stride=cols)
    density = pops[at, :]
    for q in range(1, LANES):
        density = density + pops[pl.ds(q * rows * cols + c, rows, stride=cols), :]
    m = mass[at, :]
    flag = flags[at, :]
    code = jnp.where(
        (flag == 1) & (conversion[at, :] == 1), FILLING, flag.astype(jnp.float32) + 1.0
    )
    return {
        MASS: m,
        FRAC: jnp.clip(m / density, 0.0, 1.0),
        CODE: code,
        BUB: bubble[at, :].astype(jnp.float32),
    }


def second_kernel(
    rows, cols, held, pops, mass, flags, bubble, conversion, across_even, across_odd, even_out, odd_out
):
    state = (pops, mass, flags, bubble, conversion)

    def with_rows(low, high):
        def with_cols(left_out, right_out):
            relay(rows, cols, state, low, high, left_out, right_out)

        by_parity("gy", with_cols, even_out, odd_out)

    by_parity("gx", with_rows, across_even, across_odd)


def relay(rows, cols, state, low, high, left_out, right_out):
    tall = rows + 2
    pops = state[0]
    for out, inner_col, outer_col, sign in (
        (left_out, 0, 1, -1),
        (right_out, cols - 1, cols - 2, 1),
    ):
        for c, begin, channels in (
            (inner_col, 0, list(range(CHANNELS))),
            (outer_col, CHANNELS, outer(1, sign)),
        ):
            beside = column_cells(rows, cols, c, *state)
            for k, channel in enumerate(channels):
                out[pl.ds((begin + k) * tall + 1, rows), :] = (
                    pops[pl.ds(channel * rows * cols + c, rows, stride=cols), :]
                    if channel < LANES
                    else beside[channel]
                )
        carried = (CHANNELS + len(outer(1, sign))) * tall
        spare = carried
        for halo, row, towards in ((low, 0, 1), (high, tall - 1, -1)):
            out[pl.ds(row, CHANNELS, stride=tall), :] = halo[
                pl.ds(inner_col, CHANNELS, stride=cols), :
            ]
            for k, channel in enumerate(outer(1, sign)):
                out[pl.ds((CHANNELS + k) * tall + row, 1), :] = halo[
                    pl.ds(channel * cols + outer_col, 1), :
                ]
            beyond = outer(0, towards)
            out[pl.ds(spare, len(beyond)), :] = halo[
                pl.ds(CHANNELS * cols + inner_col, len(beyond), stride=cols), :
            ]
            spare += len(beyond)
            for channel in (heading_both(towards, sign), FRAC, CODE):
                k = beyond.index(channel)
                out[pl.ds(spare, 1), :] = halo[pl.ds((CHANNELS + k) * cols + outer_col, 1), :]
                spare += 1


def side_tiles(rows):
    tall = rows + 2
    used = (CHANNELS + 7) * tall + 2 * (7 + 3)
    return -(-used // 8) * 8


def third_kernel(
    rows, cols, chunks, copies, labels,
    pops, mass_in, flags_in, bubble_in, conversion_in,
    across_even, across_odd, beside_even, beside_odd, tally, rest,
    relaxed_out, new_mass_out, gas_out,
    cells, near, sums, table, relaxed_stage, mass_stage, gas_stage, wet_sem, mass_sem, gas_sem,
):
    block = rows * cols
    tall = rows + 2
    high_rows = rows + 4
    wide = cols + 4
    total_rows = wide * high_rows

    for chunk in range(chunks):
        volume = tally[0, chunk]
        for k in range(1, copies):
            volume = volume + tally[k, chunk]
        here = min(128, labels - chunk * 128)
        gas = AMBIENT + rest[chunk] / jnp.maximum(volume, 1.0)
        gas_stage[0:1, pl.ds(chunk * 128, here)] = gas[0:1, :here]
        table[chunk] = gas
    gas_copy = pltpu.make_async_copy(gas_stage, gas_out, gas_sem)
    gas_copy.start()

    for c in range(cols):
        at = pl.ds((c + 2) * high_rows + 2, rows)
        for q in range(LANES):
            cells[q, at, :] = pops[pl.ds(q * block + c, rows, stride=cols), :]
        own = column_cells(rows, cols, c, pops, mass_in, flags_in, bubble_in, conversion_in)
        for channel, value in own.items():
            cells[channel, at, :] = value

    def fill_rows(low, high):
        for halo, inner_row, outer_row, towards in (
            (low, 1, 0, 1),
            (high, high_rows - 2, high_rows - 1, -1),
        ):
            for channel in range(CHANNELS):
                cells[channel, pl.ds(2 * high_rows + inner_row, cols, stride=high_rows), :] = halo[
                    pl.ds(channel * cols, cols), :
                ]
            for k, channel in enumerate(outer(0, towards)):
                cells[channel, pl.ds(2 * high_rows + outer_row, cols, stride=high_rows), :] = halo[
                    pl.ds((CHANNELS + k) * cols, cols), :
                ]

    def fill_cols(left, right):
        for halo, inner_col, outer_col, sign in (
            (left, 1, 0, 1),
            (right, wide - 2, wide - 1, -1),
        ):
            for channel in range(CHANNELS):
                cells[channel, pl.ds(inner_col * high_rows + 1, tall), :] = halo[
                    pl.ds(channel * tall, tall), :
                ]
            for k, channel in enumerate(outer(1, sign)):
                cells[channel, pl.ds(outer_col * high_rows + 1, tall), :] = halo[
                    pl.ds((CHANNELS + k) * tall, tall), :
                ]
            spare = (CHANNELS + 7) * tall
            for row, towards in ((0, 1), (high_rows - 1, -1)):
                for channel in outer(0, towards):
                    cells[channel, pl.ds(inner_col * high_rows + row, 1), :] = halo[
                        pl.ds(spare, 1), :
                    ]
                    spare += 1
                for channel in (heading_both(towards, sign), FRAC, CODE):
                    cells[channel, pl.ds(outer_col * high_rows + row, 1), :] = halo[
                        pl.ds(spare, 1), :
                    ]
                    spare += 1

    by_parity("gx", fill_rows, across_even, across_odd)
    by_parity("gy", fill_cols, beside_even, beside_odd)

    for begin in range(0, total_rows, 8):
        at = pl.ds(begin, min(8, total_rows - begin))
        code = cells[CODE, at, :]
        fraction = cells[FRAC, at, :]
        face = (code == FACE) | (code == FILLING)
        u = jnp.where(code == LIQUID, 1.0, jnp.where(face, 0.5 * fraction, 0.0))
        v = jnp.where(face, 0.5, 0.0)
        free = jnp.where(code == FACE, 1.0, 0.0)
        for depth in (-1, 0, 1):
            for k, value in enumerate((code, u, v)):
                near[k * 3 + depth + 1, at, :] = roll(value, depth) if depth else value
        ends = roll(free, 1) + roll(free, -1)
        near[9, at, :] = free
        near[10, at, :] = ends
        near[11, at, :] = free + ends

    def moments(tiles):
        density = tiles[0]
        for t in tiles[1:]:
            density = density + t
        flux = []
        for axis in range(3):
            plus = [tiles[q] for q in heading(axis, 1)]
            minus = [tiles[q] for q in heading(axis, -1)]
            j = plus[0] - minus[0]
            for a, b in zip(plus[1:], minus[1:]):
                j = j + (a - b)
            flux.append(j)
        inverse = 1.0 / density
        return density, [j * inverse for j in flux]

    def projection(velocity, q):
        terms = [
            velocity[axis] if VELOCITIES[q][axis] > 0 else -velocity[axis]
            for axis in range(3)
            if VELOCITIES[q][axis]
        ]
        out = terms[0]
        for t in terms[1:]:
            out = out + t
        return out

    updates, portions = [], []
    for c in range(-1, cols + 1):
        base = (c + 2) * high_rows + 1
        inside = 0 <= c < cols

        def source(array, q, base=base):
            begin = base - int(VELOCITIES[q][1]) * high_rows - int(VELOCITIES[q][0])
            return array[pl.ds(begin, tall), :]

        own = [cells[q, pl.ds(base, tall), :] for q in range(LANES)]
        mass = cells[MASS, pl.ds(base, tall), :]
        fraction = cells[FRAC, pl.ds(base, tall), :]
        code = cells[CODE, pl.ds(base, tall), :]
        bubble = cells[BUB, pl.ds(base, tall), :].astype(jnp.int32)
        gas = None
        for chunk in range(chunks):
            index = bubble - chunk * 128
            valid = (index >= 0) & (index < 128)
            found = jnp.take_along_axis(
                table[chunk, pl.ds(0, tall), :], jnp.where(valid, index, 0), axis=1
            )
            gas = found if gas is None else jnp.where(valid, found, gas)
        _, velocity = moments(own)
        still = 1.0 - 1.5 * (
            velocity[0] * velocity[0] + velocity[1] * velocity[1] + velocity[2] * velocity[2]
        )
        flow = None
        passed = [own[0]] + [None] * (LANES - 1)
        for first in range(1, LANES, 2):
            project = projection(velocity, first)
            pressed = gas * (2.0 * WEIGHTS[first]) * (still + 4.5 * project * project)
            for q in (first, first + 1):
                depth = int(VELOCITIES[q][2])
                moved = source(cells.at[q], q)
                if depth:
                    moved = roll(moved, depth)
                bounced = own[OPPOSITE[q]]
                kind = source(near.at[depth + 1], q)
                weight = source(near.at[3 + depth + 1], q) + source(near.at[6 + depth + 1], q) * fraction
                term = weight * (moved - bounced)
                flow = term if flow is None else flow + term
                passed[q] = jnp.where(
                    kind == GAS, pressed - bounced, jnp.where(kind == WALL, bounced, moved)
                )
        targets = near[10, pl.ds(base, tall), :]
        for dr in (-1, 0, 1):
            for dc in (-1, 0, 1):
                if dr or dc:
                    plane = 9 if dr and dc else 11
                    targets = targets + near[plane, pl.ds(base + dc * high_rows + dr, tall), :]
        filling = code == FILLING
        if inside:
            density, moved_velocity = moments(passed)
        else:
            density = passed[0]
            for t in passed[1:]:
                density = density + t
        taken = mass + flow
        portion = jnp.where(filling, (taken - density) / jnp.maximum(targets, 1.0), 0.0)
        portions.append(portion)
        if inside:
            updates.append(
                jnp.where(
                    code == FACE,
                    taken,
                    jnp.where((code == LIQUID) | filling, density, mass),
                )
            )
            dry = code == GAS
            still = 1.0 - 1.5 * (
                moved_velocity[0] * moved_velocity[0]
                + moved_velocity[1] * moved_velocity[1]
                + moved_velocity[2] * moved_velocity[2]
            )
            scaled = RELAX * density

            def put(q, value, own=own, c=c, dry=dry):
                relaxed_stage[pl.ds(q * tall * cols + c, tall, stride=cols), :] = jnp.where(
                    dry, own[q], value
                )

            put(0, (1.0 - RELAX) * passed[0] + (scaled * WEIGHTS[0]) * still)
            for first in range(1, LANES, 2):
                project = projection(moved_velocity, first)
                even = still + 4.5 * project * project
                odd = 3.0 * project
                share = scaled * WEIGHTS[first]
                put(first, (1.0 - RELAX) * passed[first] + share * (even + odd))
                put(first + 1, (1.0 - RELAX) * passed[first + 1] + share * (even - odd))

    relaxed_copies = [
        pltpu.make_async_copy(
            relaxed_stage.at[pl.ds((q * tall + 1) * cols, block), :],
            relaxed_out.at[pl.ds(q * block, block), :],
            wet_sem.at[q],
        )
        for q in range(LANES)
    ]
    for copy in relaxed_copies:
        copy.start()

    ends = [roll(p, 1) + roll(p, -1) for p in portions]
    full = [p + e for p, e in zip(portions, ends)]
    for c in range(cols):
        beside = ends[c + 1] + full[c] + full[c + 2]
        stacked = full[c + 1] + portions[c] + portions[c + 2]
        sums[pl.ds(8, tall), :] = stacked
        gained = beside + sums[pl.ds(7, tall), :] + sums[pl.ds(9, tall), :]
        code = cells[CODE, pl.ds((c + 2) * high_rows + 1, tall), :]
        mass_stage[pl.ds(c, tall, stride=cols), :] = jnp.where(
            code == FACE, updates[c] + gained, updates[c]
        )
    mass_copy = pltpu.make_async_copy(
        mass_stage.at[pl.ds(cols, block), :], new_mass_out, mass_sem
    )
    mass_copy.start()
    for copy in relaxed_copies:
        copy.wait()
    mass_copy.wait()
    gas_copy.wait()


def shards(gx_size, gy_size, populations, cell_mass, cell_flags, bubble, conversion, rest_volume):
    rows, cols, depth = populations.shape[1:]
    labels = rest_volume.shape[0]
    block = rows * cols
    tall = rows + 2
    devices = gx_size * gy_size
    chunks = -(-labels // 128)
    direct = devices * chunks <= 64
    copies = devices if direct else 1
    f32 = jnp.float32
    vmem = pl.BlockSpec(memory_space=pltpu.VMEM)
    hbm = pl.BlockSpec(memory_space=pltpu.HBM)

    pops = populations.reshape(LANES * block, depth)
    flat = [a.reshape(block, depth) for a in (cell_mass, cell_flags, bubble, conversion)]
    end_rows = (CHANNELS + 7) * cols
    side_rows = side_tiles(rows)

    packed = [
        (end_rows, depth),
        (end_rows, depth),
        (chunks, 8, 128),
        (copies, chunks, 8, 128),
    ]
    across_even, across_odd, rest, tally = pl.pallas_call(
        functools.partial(first_kernel, rows, cols, chunks, copies),
        out_shape=[jax.ShapeDtypeStruct(shape, f32) for shape in packed],
        in_specs=[hbm] * 6,
        out_specs=[hbm] * len(packed),
        scratch_shapes=[
            pltpu.VMEM((4 * block, depth), f32),
            pltpu.VMEM((LANES * block, depth), f32),
            pltpu.VMEM((block, depth), f32),
            pltpu.VMEM((block, depth), jnp.int32),
            pltpu.VMEM((block, depth), jnp.int32),
            pltpu.VMEM((block, depth), jnp.int32),
            pltpu.VMEM((1, labels), f32),
            pltpu.SemaphoreType.DMA((6,)),
        ]
        + [pltpu.VMEM(shape, f32) for shape in packed]
        + [pltpu.SemaphoreType.DMA((len(packed),))],
        cost_estimate=pl.CostEstimate(flops=2000000, bytes_accessed=2000000, transcendentals=0),
        compiler_params=pltpu.CompilerParams(vmem_limit_bytes=67043328),
        name="pack",
    )(pops, *flat, rest_volume.reshape(1, labels))

    held = pl.pallas_call(
        lambda out: out.__setitem__(Ellipsis, jnp.zeros((8, 128), f32)),
        out_shape=jax.ShapeDtypeStruct((8, 128), f32),
        out_specs=vmem,
        cost_estimate=pl.CostEstimate(flops=HOLD, bytes_accessed=4096, transcendentals=0),
        compiler_params=pltpu.CompilerParams(vmem_limit_bytes=1 << 20),
        name="pause",
    )()

    def swapped(x, axis, size, odd):
        return lax.ppermute(x, axis, paired(size, odd))

    across_odd = swapped(across_odd, "gx", gx_size, True)
    across_even = swapped(across_even, "gx", gx_size, False)
    if direct:
        tallies = lax.all_to_all(
            tally.reshape(devices, chunks * 8, 128), ("gx", "gy"), 0, 0
        ).reshape(devices, chunks, 8, 128)
    else:
        tallies = lax.psum(tally[0, :, 0], ("gx", "gy"))
        tallies = jnp.broadcast_to(tallies[None, :, None, :], (1, chunks, 8, 128))

    beside_even, beside_odd = pl.pallas_call(
        functools.partial(second_kernel, rows, cols),
        out_shape=[jax.ShapeDtypeStruct((side_rows, depth), f32)] * 2,
        in_specs=[vmem] * 8,
        out_specs=[vmem] * 2,
        compiler_params=pltpu.CompilerParams(vmem_limit_bytes=4 << 20),
        name="relay",
    )(held, pops, *flat, across_even, across_odd)
    beside_odd = swapped(beside_odd, "gy", gy_size, True)
    beside_even = swapped(beside_even, "gy", gy_size, False)

    relaxed, new_mass, gas = pl.pallas_call(
        functools.partial(third_kernel, rows, cols, chunks, copies, labels),
        out_shape=[
            jax.ShapeDtypeStruct((LANES * block, depth), f32),
            jax.ShapeDtypeStruct((block, depth), f32),
            jax.ShapeDtypeStruct((1, labels), f32),
        ],
        in_specs=[vmem] * 11,
        out_specs=[
            pl.BlockSpec(memory_space=pl.ANY),
            pl.BlockSpec(memory_space=pl.ANY),
            pl.BlockSpec(memory_space=pl.ANY),
        ],
        scratch_shapes=[
            pltpu.VMEM((CHANNELS, (cols + 4) * (rows + 4), depth), f32),
            pltpu.VMEM((12, (cols + 4) * (rows + 4), depth), f32),
            pltpu.VMEM((24, depth), f32),
            pltpu.VMEM((chunks, 8, 128), f32),
            pltpu.VMEM((LANES * tall * cols, depth), f32),
            pltpu.VMEM((tall * cols, depth), f32),
            pltpu.VMEM((1, labels), f32),
            pltpu.SemaphoreType.DMA((LANES,)),
            pltpu.SemaphoreType.DMA,
            pltpu.SemaphoreType.DMA,
        ],
        cost_estimate=pl.CostEstimate(flops=5000000, bytes_accessed=3000000, transcendentals=0),
        compiler_params=pltpu.CompilerParams(vmem_limit_bytes=12 << 20),
        name="settle",
    )(pops, *flat, across_even, across_odd, beside_even, beside_odd, tallies, rest)
    return (
        relaxed.reshape(LANES, rows, cols, depth),
        new_mass.reshape(rows, cols, depth),
        gas.reshape(labels),
    )


def solution(mesh):
    placed = (
        P(None, "gx", "gy", None),
        P("gx", "gy", None),
        P("gx", "gy", None),
        P("gx", "gy", None),
        P("gx", "gy", None),
        P(),
    )

    def step(*args):
        return shards(mesh.shape["gx"], mesh.shape["gy"], *args)

    return jax.shard_map(
        step,
        mesh=mesh,
        in_specs=placed,
        out_specs=(P(None, "gx", "gy", None), P("gx", "gy", None), P()),
        check_vma=False,
    )
```

```python
import functools

import jax
import jax.numpy as jnp
import numpy as np
from jax import lax
from jax.experimental import pallas as pl
from jax.experimental.pallas import tpu as pltpu
from jax.sharding import PartitionSpec as P


VELOCITIES = np.array(
    [
        [0, 0, 0],
        [1, 0, 0],
        [-1, 0, 0],
        [0, 1, 0],
        [0, -1, 0],
        [0, 0, 1],
        [0, 0, -1],
        [1, 1, 0],
        [-1, -1, 0],
        [1, -1, 0],
        [-1, 1, 0],
        [1, 0, 1],
        [-1, 0, -1],
        [1, 0, -1],
        [-1, 0, 1],
        [0, 1, 1],
        [0, -1, -1],
        [0, 1, -1],
        [0, -1, 1],
    ]
)
OPPOSITE = [0, 2, 1, 4, 3, 6, 5, 8, 7, 10, 9, 12, 11, 14, 13, 16, 15, 18, 17]
WEIGHTS = [1.0 / 3.0] + [1.0 / 18.0] * 6 + [1.0 / 36.0] * 12
RELAX = 1.0 / 0.6
AMBIENT = 2.0
HOLD = 2000000000
LANES = 19
MASS, FRAC, CODE, BUB = 19, 20, 21, 22
CHANNELS = 23
WALL, GAS, FACE, LIQUID, FILLING = 0.0, 1.0, 2.0, 3.0, 5.0


def heading(axis, sign):
    return [q for q in range(LANES) if VELOCITIES[q][axis] == sign]


def heading_both(rows, cols):
    return [q for q in range(LANES) if VELOCITIES[q][0] == rows and VELOCITIES[q][1] == cols][0]


def outer(axis, sign):
    return heading(axis, sign) + [FRAC, CODE]


def roll(x, shift):
    return pltpu.roll(x, shift % x.shape[-1], x.ndim - 1)


def by_parity(axis, use, even, odd):
    odd_device = lax.rem(lax.axis_index(axis), 2) == 1

    @pl.when(odd_device)
    def _():
        use(even, odd)

    @pl.when(jnp.logical_not(odd_device))
    def _():
        use(odd, even)


def paired(size, odd):
    pairs = []
    for i in range(1 if odd else 0, size - 1, 2):
        pairs += [(i, i + 1), (i + 1, i)]
    return pairs


def first_kernel(
    rows, cols, chunks, copies,
    pops_in, mass_in, flags_in, bubble_in, conversion_in,
    across_even_out, across_odd_out, tally_out,
    aux, pops, mass, flags, bubble, conversion, sems,
    across_even, across_odd, tally, out_sems,
):
    block = rows * cols
    copies_in = [
        pltpu.make_async_copy(a, b, sems.at[k])
        for k, (a, b) in enumerate(
            (
                (pops_in, pops),
                (mass_in, mass),
                (flags_in, flags),
                (bubble_in, bubble),
                (conversion_in, conversion),
            )
        )
    ]
    for copy in copies_in:
        copy.start()
    for copy in copies_in:
        copy.wait()
    sent = []

    def send(k, staged, out):
        copy = pltpu.make_async_copy(staged, out, out_sems.at[k])
        copy.start()
        sent.append(copy)

    contributions = []
    lane_count = mass.shape[-1]
    label_rows = lax.broadcasted_iota(jnp.int32, (128, lane_count), 0)

    def count_row(total, r, chunk):
        for c in range(cols):
            row = bubble[pl.ds(r * cols + c, 1), :]
            term = contributions[r][c : c + 1, :]
            total = total + jnp.where(label_rows + chunk * 128 == row, term, 0.0)
        return total

    for r in range(rows):
        at = pl.ds(r * cols, cols)
        density = pops[0, at, :]
        for q in range(1, LANES):
            density = density + pops[q, at, :]
        m = mass[at, :]
        flag = flags[at, :]
        fraction = jnp.clip(m / density, 0.0, 1.0)
        code = jnp.where(
            (flag == 1) & (conversion[at, :] == 1), FILLING, flag.astype(jnp.float32) + 1.0
        )
        aux[at, :] = m
        aux[pl.ds(block + r * cols, cols), :] = fraction
        aux[pl.ds(2 * block + r * cols, cols), :] = code
        aux[pl.ds(3 * block + r * cols, cols), :] = bubble[at, :].astype(jnp.float32)
        contributions.append(
            jnp.where(flag == 0, 1.0, jnp.where(flag == 1, 1.0 - fraction, 0.0))
        )

    def tile(channel, r):
        if channel < LANES:
            return pops[channel, pl.ds(r * cols, cols), :]
        return aux[pl.ds((channel - LANES) * block + r * cols, cols), :]

    def send_rows(out, inner_row, outer_row, sign):
        for channel in range(CHANNELS):
            out[pl.ds(channel * cols, cols), :] = tile(channel, inner_row)
        for k, channel in enumerate(outer(0, sign)):
            out[pl.ds((CHANNELS + k) * cols, cols), :] = tile(channel, outer_row)

    def low_high(low, high):
        send_rows(low, 0, 1, -1)
        send_rows(high, rows - 1, rows - 2, 1)

    by_parity("gx", low_high, across_even, across_odd)
    send(0, across_even, across_even_out)
    send(1, across_odd, across_odd_out)


    def count(chunk):
        total = jnp.zeros((128, lane_count), jnp.float32)
        for r in range(rows):
            total = count_row(total, r, chunk)
        return lax.dot_general(
            jnp.ones((8, lane_count), jnp.float32),
            total,
            (((1,), (1,)), ((), ())),
            precision=lax.Precision.HIGHEST,
            preferred_element_type=jnp.float32,
        )

    for chunk in range(chunks):
        summed = count(chunk)
        for k in range(copies):
            tally[k, chunk] = summed
    send(2, tally, tally_out)
    for copy in sent:
        copy.wait()


def column_cells(rows, cols, c, pops, mass, flags, bubble, conversion):
    at = pl.ds(c, rows, stride=cols)
    density = pops[at, :]
    for q in range(1, LANES):
        density = density + pops[pl.ds(q * rows * cols + c, rows, stride=cols), :]
    m = mass[at, :]
    flag = flags[at, :]
    code = jnp.where(
        (flag == 1) & (conversion[at, :] == 1), FILLING, flag.astype(jnp.float32) + 1.0
    )
    return {
        MASS: m,
        FRAC: jnp.clip(m / density, 0.0, 1.0),
        CODE: code,
        BUB: bubble[at, :].astype(jnp.float32),
    }


def second_kernel(
    rows, cols, held, pops, mass, flags, bubble, conversion, across_even, across_odd,
    even_out, odd_out,
):
    state = (pops, mass, flags, bubble, conversion)

    def with_rows(low, high):
        def with_cols(left_out, right_out):
            relay(rows, cols, state, low, high, left_out, right_out)

        by_parity("gy", with_cols, even_out, odd_out)

    by_parity("gx", with_rows, across_even, across_odd)


def relay(rows, cols, state, low, high, left_out, right_out):
    tall = rows + 2
    pops = state[0]
    for out, inner_col, outer_col, sign in (
        (left_out, 0, 1, -1),
        (right_out, cols - 1, cols - 2, 1),
    ):
        for c, begin, channels in (
            (inner_col, 0, list(range(CHANNELS))),
            (outer_col, CHANNELS, outer(1, sign)),
        ):
            beside = column_cells(rows, cols, c, *state)
            for k, channel in enumerate(channels):
                out[pl.ds((begin + k) * tall + 1, rows), :] = (
                    pops[pl.ds(channel * rows * cols + c, rows, stride=cols), :]
                    if channel < LANES
                    else beside[channel]
                )
        carried = (CHANNELS + len(outer(1, sign))) * tall
        spare = carried
        for halo, row, towards in ((low, 0, 1), (high, tall - 1, -1)):
            out[pl.ds(row, CHANNELS, stride=tall), :] = halo[
                pl.ds(inner_col, CHANNELS, stride=cols), :
            ]
            for k, channel in enumerate(outer(1, sign)):
                out[pl.ds((CHANNELS + k) * tall + row, 1), :] = halo[
                    pl.ds(channel * cols + outer_col, 1), :
                ]
            beyond = outer(0, towards)
            out[pl.ds(spare, len(beyond)), :] = halo[
                pl.ds(CHANNELS * cols + inner_col, len(beyond), stride=cols), :
            ]
            spare += len(beyond)
            for channel in (heading_both(towards, sign), FRAC, CODE):
                k = beyond.index(channel)
                out[pl.ds(spare, 1), :] = halo[pl.ds((CHANNELS + k) * cols + outer_col, 1), :]
                spare += 1


def side_tiles(rows):
    tall = rows + 2
    used = (CHANNELS + 7) * tall + 2 * (7 + 3)
    return -(-used // 8) * 8


def inner_columns(cols):
    return list(range(1, cols - 1))


def edge_columns(cols):
    return [-1, 0, cols - 1, cols]


def third_kernel(rows, cols, edges, *refs):
    pops, mass_in, flags_in, bubble_in, conversion_in, across_even, across_odd = refs[:7]
    sides = refs[7:9] if edges else ()
    fixed, scaling, linear, kept, cells, near = refs[-6:]
    if not edges:
        rest, rest_table = refs[7], refs[-7]
        labels_all = rest.shape[-1]
        for chunk in range(-(-labels_all // 128)):
            here = min(128, labels_all - chunk * 128)
            rest_table[chunk, :, pl.ds(0, here)] = jnp.broadcast_to(
                rest[0:1, pl.ds(chunk * 128, here)], (8, here)
            )
    todo = edge_columns(cols) if edges else inner_columns(cols)
    stored = [c for c in todo if 0 <= c < cols]
    block = rows * cols
    tall = rows + 2
    high_rows = rows + 4
    wide = cols + 4
    total_rows = wide * high_rows

    for c in (0, 1, cols - 2, cols - 1) if edges else range(cols):
        at = pl.ds((c + 2) * high_rows + 2, rows)
        for q in range(LANES):
            cells[q, at, :] = pops[pl.ds(q * block + c, rows, stride=cols), :]
        own = column_cells(rows, cols, c, pops, mass_in, flags_in, bubble_in, conversion_in)
        for channel, value in own.items():
            cells[channel, at, :] = value

    def fill_rows(low, high):
        for halo, inner_row, outer_row, towards in (
            (low, 1, 0, 1),
            (high, high_rows - 2, high_rows - 1, -1),
        ):
            for channel in range(CHANNELS):
                cells[channel, pl.ds(2 * high_rows + inner_row, cols, stride=high_rows), :] = halo[
                    pl.ds(channel * cols, cols), :
                ]
            for k, channel in enumerate(outer(0, towards)):
                cells[channel, pl.ds(2 * high_rows + outer_row, cols, stride=high_rows), :] = halo[
                    pl.ds((CHANNELS + k) * cols, cols), :
                ]

    def fill_cols(left, right):
        for halo, inner_col, outer_col, sign in (
            (left, 1, 0, 1),
            (right, wide - 2, wide - 1, -1),
        ):
            for channel in range(CHANNELS):
                cells[channel, pl.ds(inner_col * high_rows + 1, tall), :] = halo[
                    pl.ds(channel * tall, tall), :
                ]
            for k, channel in enumerate(outer(1, sign)):
                cells[channel, pl.ds(outer_col * high_rows + 1, tall), :] = halo[
                    pl.ds((CHANNELS + k) * tall, tall), :
                ]
            spare = (CHANNELS + 7) * tall
            for row, towards in ((0, 1), (high_rows - 1, -1)):
                for channel in outer(0, towards):
                    cells[channel, pl.ds(inner_col * high_rows + row, 1), :] = halo[
                        pl.ds(spare, 1), :
                    ]
                    spare += 1
                for channel in (heading_both(towards, sign), FRAC, CODE):
                    cells[channel, pl.ds(outer_col * high_rows + row, 1), :] = halo[
                        pl.ds(spare, 1), :
                    ]
                    spare += 1

    by_parity("gx", fill_rows, across_even, across_odd)
    if edges:
        by_parity("gy", fill_cols, *sides)

    if edges:
        spans = ((0, 4 * high_rows), (total_rows - 4 * high_rows, total_rows))
    else:
        spans = ((2 * high_rows, total_rows - 2 * high_rows),)
    for begin, end in [(b, min(b + 8, e)) for low, e in spans for b in range(low, e, 8)]:
        at = pl.ds(begin, end - begin)
        code = cells[CODE, at, :]
        fraction = cells[FRAC, at, :]
        face = (code == FACE) | (code == FILLING)
        u = jnp.where(code == LIQUID, 1.0, jnp.where(face, 0.5 * fraction, 0.0))
        v = jnp.where(face, 0.5, 0.0)
        free = jnp.where(code == FACE, 1.0, 0.0)
        for depth in (-1, 0, 1):
            for k, value in enumerate((code, u, v)):
                near[k * 3 + depth + 1, at, :] = roll(value, depth) if depth else value
        ends = roll(free, 1) + roll(free, -1)
        near[9, at, :] = free
        near[10, at, :] = ends
        near[11, at, :] = free + ends

    for slot, c in enumerate(todo):
        base = (c + 2) * high_rows + 1
        inside = 0 <= c < cols
        out = pl.ds(slot * tall, tall)
        column = pl.ds(stored.index(c) * tall if inside else 0, tall)

        def source(array, q, base=base):
            begin = base - int(VELOCITIES[q][1]) * high_rows - int(VELOCITIES[q][0])
            return array[pl.ds(begin, tall), :]

        own = [cells[q, pl.ds(base, tall), :] for q in range(LANES)]
        mass = cells[MASS, pl.ds(base, tall), :]
        fraction = cells[FRAC, pl.ds(base, tall), :]
        code = cells[CODE, pl.ds(base, tall), :]
        dry = code == GAS
        density = total(own)
        inverse = 1.0 / density
        velocity = [j * inverse for j in momentum(own)]
        still = rest_part(velocity)
        flow = None
        constant = [own[0]] + [None] * (LANES - 1)
        factor = [None] * LANES
        for first in range(1, LANES, 2):
            project = projection(velocity, first)
            pressed = (2.0 * WEIGHTS[first]) * (still + 4.5 * project * project)
            for q in (first, first + 1):
                depth = int(VELOCITIES[q][2])
                moved = source(cells.at[q], q)
                if depth:
                    moved = roll(moved, depth)
                bounced = own[OPPOSITE[q]]
                kind = source(near.at[depth + 1], q)
                weight = source(near.at[3 + depth + 1], q) + source(near.at[6 + depth + 1], q) * fraction
                term = weight * (moved - bounced)
                flow = term if flow is None else flow + term
                gas_side = kind == GAS
                constant[q] = jnp.where(
                    gas_side, -bounced, jnp.where(kind == WALL, bounced, moved)
                )
                factor[q] = jnp.where(gas_side, pressed, 0.0)
        targets = near[10, pl.ds(base, tall), :]
        for dr in (-1, 0, 1):
            for dc in (-1, 0, 1):
                if dr or dc:
                    plane = 9 if dr and dc else 11
                    targets = targets + near[plane, pl.ds(base + dc * high_rows + dr, tall), :]
        linear[0, out, :] = total(constant)
        linear[1, out, :] = total(factor[1:])
        kept[0, out, :] = mass + flow
        kept[1, out, :] = jnp.maximum(targets, 1.0)
        kept[2, out, :] = code
        kept[3, out, :] = cells[BUB, pl.ds(base, tall), :]
        if inside:
            kept[4, out, :] = mass
            for axis, j in enumerate(momentum(constant)):
                linear[2 + axis, out, :] = j
            for axis, j in enumerate(momentum(factor)):
                linear[5 + axis, out, :] = j
            for q in range(LANES):
                fixed[q, column, :] = jnp.where(dry, own[q], (1.0 - RELAX) * constant[q])
                if q:
                    scaling[q - 1, column, :] = jnp.where(dry, 0.0, (1.0 - RELAX) * factor[q])


def total(tiles):
    out = tiles[0]
    for t in tiles[1:]:
        out = out + t
    return out


def momentum(tiles):
    flux = []
    for axis in range(3):
        plus = [tiles[q] for q in heading(axis, 1)]
        minus = [tiles[q] for q in heading(axis, -1)]
        j = plus[0] - minus[0]
        for a, b in zip(plus[1:], minus[1:]):
            j = j + (a - b)
        flux.append(j)
    return flux


def rest_part(velocity):
    return 1.0 - 1.5 * (
        velocity[0] * velocity[0] + velocity[1] * velocity[1] + velocity[2] * velocity[2]
    )


def projection(velocity, q):
    terms = [
        velocity[axis] if VELOCITIES[q][axis] > 0 else -velocity[axis]
        for axis in range(3)
        if VELOCITIES[q][axis]
    ]
    return total(terms)


def fourth_kernel(
    rows, cols, chunks, copies, labels,
    inner_fixed, inner_scaling, inner_linear, inner_kept,
    edge_fixed, edge_scaling, edge_linear, edge_kept, tally, rest,
    relaxed_out, new_mass_out, gas_out,
    sums, table, relaxed_stage, mass_stage, gas_stage, wet_sem, mass_sem, gas_sem,
):
    block = rows * cols
    tall = rows + 2
    for chunk in range(chunks):
        volume = tally[0, chunk]
        for k in range(1, copies):
            volume = volume + tally[k, chunk]
        here = min(128, labels - chunk * 128)
        gas = AMBIENT + rest[chunk] / jnp.maximum(volume, 1.0)
        gas_stage[0:1, pl.ds(chunk * 128, here)] = gas[0:1, :here]
        table[chunk] = gas
    gas_copy = pltpu.make_async_copy(gas_stage, gas_out, gas_sem)
    gas_copy.start()

    def place(c):
        if c in inner_columns(cols):
            slot = inner_columns(cols).index(c)
            parts = (inner_fixed, inner_scaling, inner_linear, inner_kept)
            return parts, pl.ds(slot * tall, tall), pl.ds(slot * tall, tall)
        slot = edge_columns(cols).index(c)
        parts = (edge_fixed, edge_scaling, edge_linear, edge_kept)
        return parts, pl.ds(slot * tall, tall), pl.ds((0 if c <= 0 else 1) * tall, tall)

    def settled(c):
        (_, _, linear, kept), at, _ = place(c)
        code = kept[2, at, :]
        bubble = kept[3, at, :].astype(jnp.int32)
        gas = None
        for chunk in range(chunks):
            index = bubble - chunk * 128
            valid = (index >= 0) & (index < 128)
            found = jnp.take_along_axis(
                table[chunk, pl.ds(0, tall), :], jnp.where(valid, index, 0), axis=1
            )
            gas = found if gas is None else jnp.where(valid, found, gas)
        density = linear[0, at, :] + gas * linear[1, at, :]
        portion = jnp.where(
            code == FILLING, (kept[0, at, :] - density) / kept[1, at, :], 0.0
        )
        return at, code, gas, density, portion

    updates, portions, states = [], [], []
    for c in range(cols):
        _, code, gas, density, portion = settled(c)
        (_, _, linear, kept), at, _ = place(c)
        portions.append(portion)
        dry = code == GAS
        updates.append(
            jnp.where(
                code == FACE,
                kept[0, at, :],
                jnp.where(dry, kept[4, at, :], density),
            )
        )
        inverse = 1.0 / jnp.where(dry, 1.0, density)
        velocity = [
            (linear[2 + axis, at, :] + gas * linear[5 + axis, at, :]) * inverse for axis in range(3)
        ]
        states.append((gas, velocity, rest_part(velocity), jnp.where(dry, 0.0, RELAX * density)))

    relaxed_copies = []

    def leave(q):
        copy = pltpu.make_async_copy(
            relaxed_stage.at[pl.ds((q * tall + 1) * cols, block), :],
            relaxed_out.at[pl.ds(q * block, block), :],
            wet_sem.at[q],
        )
        copy.start()
        relaxed_copies.append(copy)

    def put(q, c, value):
        relaxed_stage[pl.ds(q * tall * cols + c, tall, stride=cols), :] = value

    for c, (_, _, still, scaled) in enumerate(states):
        (fixed, _, _, _), _, column = place(c)
        put(0, c, fixed[0, column, :] + (scaled * WEIGHTS[0]) * still)
    leave(0)
    for first in range(1, LANES, 2):
        for c, (gas, velocity, still, scaled) in enumerate(states):
            (fixed, scaling, _, _), _, column = place(c)
            project = projection(velocity, first)
            even = still + 4.5 * project * project
            odd = 3.0 * project
            share = scaled * WEIGHTS[first]
            for q, part in ((first, even + odd), (first + 1, even - odd)):
                put(q, c, fixed[q, column, :] + gas * scaling[q - 1, column, :] + share * part)
        leave(first)
        leave(first + 1)

    portions = [settled(-1)[-1]] + portions + [settled(cols)[-1]]
    ends = [roll(p, 1) + roll(p, -1) for p in portions]
    full = [p + e for p, e in zip(portions, ends)]
    for c in range(cols):
        beside = ends[c + 1] + full[c] + full[c + 2]
        stacked = full[c + 1] + portions[c] + portions[c + 2]
        sums[pl.ds(8, tall), :] = stacked
        gained = beside + sums[pl.ds(7, tall), :] + sums[pl.ds(9, tall), :]
        (_, _, _, kept), at, _ = place(c)
        code = kept[2, at, :]
        mass_stage[pl.ds(c, tall, stride=cols), :] = jnp.where(
            code == FACE, updates[c] + gained, updates[c]
        )
    mass_copy = pltpu.make_async_copy(
        mass_stage.at[pl.ds(cols, block), :], new_mass_out, mass_sem
    )
    mass_copy.start()
    for copy in relaxed_copies:
        copy.wait()
    mass_copy.wait()
    gas_copy.wait()


def shards(gx_size, gy_size, populations, cell_mass, cell_flags, bubble, conversion, rest_volume):
    rows, cols, depth = populations.shape[1:]
    labels = rest_volume.shape[0]
    block = rows * cols
    tall = rows + 2
    devices = gx_size * gy_size
    chunks = -(-labels // 128)
    direct = devices * chunks <= 64
    copies = devices if direct else 1
    f32 = jnp.float32
    vmem = pl.BlockSpec(memory_space=pltpu.VMEM)
    hbm = pl.BlockSpec(memory_space=pltpu.HBM)

    pops = populations.reshape(LANES * block, depth)
    flat = [a.reshape(block, depth) for a in (cell_mass, cell_flags, bubble, conversion)]
    end_rows = (CHANNELS + 7) * cols
    side_rows = side_tiles(rows)

    packed = [
        (end_rows, depth),
        (end_rows, depth),
        (copies, chunks, 8, 128),
    ]
    across_even, across_odd, tally = pl.pallas_call(
        functools.partial(first_kernel, rows, cols, chunks, copies),
        out_shape=[jax.ShapeDtypeStruct(shape, f32) for shape in packed],
        in_specs=[hbm] * 5,
        out_specs=[hbm] * len(packed),
        scratch_shapes=[
            pltpu.VMEM((4 * block, depth), f32),
            pltpu.VMEM((LANES, block, depth), f32),
            pltpu.VMEM((block, depth), f32),
            pltpu.VMEM((block, depth), jnp.int32),
            pltpu.VMEM((block, depth), jnp.int32),
            pltpu.VMEM((block, depth), jnp.int32),
            pltpu.SemaphoreType.DMA((5,)),
        ]
        + [pltpu.VMEM(shape, f32) for shape in packed]
        + [pltpu.SemaphoreType.DMA((len(packed),))],
        cost_estimate=pl.CostEstimate(flops=2000000, bytes_accessed=2000000, transcendentals=0),
        compiler_params=pltpu.CompilerParams(vmem_limit_bytes=67043328),
        name="pack",
    )(populations.reshape(LANES, block, depth), *flat)

    held = pl.pallas_call(
        lambda out: out.__setitem__(Ellipsis, jnp.zeros((8, 128), f32)),
        out_shape=jax.ShapeDtypeStruct((8, 128), f32),
        out_specs=vmem,
        cost_estimate=pl.CostEstimate(flops=HOLD, bytes_accessed=4096, transcendentals=0),
        compiler_params=pltpu.CompilerParams(vmem_limit_bytes=1 << 20),
        name="pause",
    )()

    def swapped(x, axis, size, odd):
        return lax.ppermute(x, axis, paired(size, odd))

    across_odd = swapped(across_odd, "gx", gx_size, True)
    across_even = swapped(across_even, "gx", gx_size, False)
    if direct:
        tallies = lax.all_to_all(
            tally.reshape(devices, chunks * 8, 128), ("gx", "gy"), 0, 0
        ).reshape(devices, chunks, 8, 128)
    else:
        tallies = lax.psum(tally[0, :, 0], ("gx", "gy"))
        tallies = jnp.broadcast_to(tallies[None, :, None, :], (1, chunks, 8, 128))

    beside_even, beside_odd = pl.pallas_call(
        functools.partial(second_kernel, rows, cols),
        out_shape=[jax.ShapeDtypeStruct((side_rows, depth), f32)] * 2,
        in_specs=[vmem] * 8,
        out_specs=[vmem] * 2,
        compiler_params=pltpu.CompilerParams(vmem_limit_bytes=4 << 20),
        name="relay",
    )(held, pops, *flat, across_even, across_odd)
    beside_odd = swapped(beside_odd, "gy", gy_size, True)
    beside_even = swapped(beside_even, "gy", gy_size, False)

    def prepare(edges, *sides):
        todo = edge_columns(cols) if edges else inner_columns(cols)
        stored = [c for c in todo if 0 <= c < cols]
        prepared = [
            (LANES, len(stored) * tall, depth),
            (LANES - 1, len(stored) * tall, depth),
            (8, len(todo) * tall, depth),
            (5, len(todo) * tall, depth),
        ]
        if not edges:
            prepared.insert(0, (chunks, 8, 128))
        return pl.pallas_call(
            functools.partial(third_kernel, rows, cols, edges),
            out_shape=[jax.ShapeDtypeStruct(shape, f32) for shape in prepared],
            in_specs=[vmem] * (7 + len(sides)),
            out_specs=[vmem] * len(prepared),
            scratch_shapes=[
                pltpu.VMEM((CHANNELS, (cols + 4) * (rows + 4), depth), f32),
                pltpu.VMEM((12, (cols + 4) * (rows + 4), depth), f32),
            ],
            cost_estimate=pl.CostEstimate(flops=5000000, bytes_accessed=3000000, transcendentals=0),
            compiler_params=pltpu.CompilerParams(vmem_limit_bytes=8 << 20),
            name="edges" if edges else "inner",
        )(pops, *flat, across_even, across_odd, *sides)

    rest, *inner = prepare(False, rest_volume.reshape(1, labels))
    edge = prepare(True, beside_even, beside_odd)
    relaxed, new_mass, gas = pl.pallas_call(
        functools.partial(fourth_kernel, rows, cols, chunks, copies, labels),
        out_shape=[
            jax.ShapeDtypeStruct((LANES * block, depth), f32),
            jax.ShapeDtypeStruct((block, depth), f32),
            jax.ShapeDtypeStruct((1, labels), f32),
        ],
        in_specs=[vmem] * 10,
        out_specs=[pl.BlockSpec(memory_space=pl.ANY)] * 3,
        scratch_shapes=[
            pltpu.VMEM((24, depth), f32),
            pltpu.VMEM((chunks, 8, 128), f32),
            pltpu.VMEM((LANES * tall * cols, depth), f32),
            pltpu.VMEM((tall * cols, depth), f32),
            pltpu.VMEM((1, labels), f32),
            pltpu.SemaphoreType.DMA((LANES,)),
            pltpu.SemaphoreType.DMA,
            pltpu.SemaphoreType.DMA,
        ],
        cost_estimate=pl.CostEstimate(flops=2000000, bytes_accessed=3000000, transcendentals=0),
        compiler_params=pltpu.CompilerParams(vmem_limit_bytes=12 << 20),
        name="settle",
    )(*inner, *edge, tallies, rest)
    return (
        relaxed.reshape(LANES, rows, cols, depth),
        new_mass.reshape(rows, cols, depth),
        gas.reshape(labels),
    )


def solution(mesh):
    placed = (
        P(None, "gx", "gy", None),
        P("gx", "gy", None),
        P("gx", "gy", None),
        P("gx", "gy", None),
        P("gx", "gy", None),
        P(),
    )

    def step(*args):
        return shards(mesh.shape["gx"], mesh.shape["gy"], *args)

    return jax.shard_map(
        step,
        mesh=mesh,
        in_specs=placed,
        out_specs=(P(None, "gx", "gy", None), P("gx", "gy", None), P()),
        check_vma=False,
    )
```

```python
import functools

import jax
import jax.numpy as jnp
import numpy as np
from jax import lax
from jax.experimental import pallas as pl
from jax.experimental.pallas import tpu as pltpu
from jax.sharding import PartitionSpec as P


VELOCITIES = np.array(
    [
        [0, 0, 0],
        [1, 0, 0],
        [-1, 0, 0],
        [0, 1, 0],
        [0, -1, 0],
        [0, 0, 1],
        [0, 0, -1],
        [1, 1, 0],
        [-1, -1, 0],
        [1, -1, 0],
        [-1, 1, 0],
        [1, 0, 1],
        [-1, 0, -1],
        [1, 0, -1],
        [-1, 0, 1],
        [0, 1, 1],
        [0, -1, -1],
        [0, 1, -1],
        [0, -1, 1],
    ]
)
OPPOSITE = [0, 2, 1, 4, 3, 6, 5, 8, 7, 10, 9, 12, 11, 14, 13, 16, 15, 18, 17]
WEIGHTS = [1.0 / 3.0] + [1.0 / 18.0] * 6 + [1.0 / 36.0] * 12
RELAX = 1.0 / 0.6
AMBIENT = 2.0
HOLD = 2000000000
LANES = 19
MASS, FRAC, CODE, BUB = 19, 20, 21, 22
CHANNELS = 23
WALL, GAS, FACE, LIQUID, FILLING = 0.0, 1.0, 2.0, 3.0, 5.0


def heading(axis, sign):
    return [q for q in range(LANES) if VELOCITIES[q][axis] == sign]


def heading_both(rows, cols):
    return [q for q in range(LANES) if VELOCITIES[q][0] == rows and VELOCITIES[q][1] == cols][0]


def outer(axis, sign):
    return heading(axis, sign) + [FRAC, CODE]


def roll(x, shift):
    return pltpu.roll(x, shift % x.shape[-1], x.ndim - 1)


def by_parity(axis, use, even, odd):
    odd_device = lax.rem(lax.axis_index(axis), 2) == 1

    @pl.when(odd_device)
    def _():
        use(even, odd)

    @pl.when(jnp.logical_not(odd_device))
    def _():
        use(odd, even)


def paired(size, odd):
    pairs = []
    for i in range(1 if odd else 0, size - 1, 2):
        pairs += [(i, i + 1), (i + 1, i)]
    return pairs


def first_kernel(
    rows, cols, chunks, copies,
    pops_in, mass_in, flags_in, bubble_in, conversion_in,
    across_even_out, across_odd_out, tally_out,
    aux, pops, mass, flags, bubble, conversion, sems,
    across_even, across_odd, tally, out_sems,
):
    block = rows * cols
    copies_in = [
        pltpu.make_async_copy(a, b, sems.at[k])
        for k, (a, b) in enumerate(
            (
                (pops_in, pops),
                (mass_in, mass),
                (flags_in, flags),
                (bubble_in, bubble),
                (conversion_in, conversion),
            )
        )
    ]
    for copy in copies_in:
        copy.start()
    for copy in copies_in:
        copy.wait()
    sent = []

    def send(k, staged, out):
        copy = pltpu.make_async_copy(staged, out, out_sems.at[k])
        copy.start()
        sent.append(copy)

    contributions = []
    lane_count = mass.shape[-1]
    label_rows = lax.broadcasted_iota(jnp.int32, (128, lane_count), 0)

    def count_row(total, r, chunk):
        for c in range(cols):
            row = bubble[pl.ds(r * cols + c, 1), :]
            term = contributions[r][c : c + 1, :]
            total = total + jnp.where(label_rows + chunk * 128 == row, term, 0.0)
        return total

    for r in range(rows):
        at = pl.ds(r * cols, cols)
        density = pops[0, at, :]
        for q in range(1, LANES):
            density = density + pops[q, at, :]
        m = mass[at, :]
        flag = flags[at, :]
        fraction = jnp.clip(m / density, 0.0, 1.0)
        code = jnp.where(
            (flag == 1) & (conversion[at, :] == 1), FILLING, flag.astype(jnp.float32) + 1.0
        )
        aux[at, :] = m
        aux[pl.ds(block + r * cols, cols), :] = fraction
        aux[pl.ds(2 * block + r * cols, cols), :] = code
        aux[pl.ds(3 * block + r * cols, cols), :] = bubble[at, :].astype(jnp.float32)
        contributions.append(
            jnp.where(flag == 0, 1.0, jnp.where(flag == 1, 1.0 - fraction, 0.0))
        )

    def tile(channel, r):
        if channel < LANES:
            return pops[channel, pl.ds(r * cols, cols), :]
        return aux[pl.ds((channel - LANES) * block + r * cols, cols), :]

    def send_rows(out, inner_row, outer_row, sign):
        for channel in range(CHANNELS):
            out[pl.ds(channel * cols, cols), :] = tile(channel, inner_row)
        for k, channel in enumerate(outer(0, sign)):
            out[pl.ds((CHANNELS + k) * cols, cols), :] = tile(channel, outer_row)

    def low_high(low, high):
        send_rows(low, 0, 1, -1)
        send_rows(high, rows - 1, rows - 2, 1)

    by_parity("gx", low_high, across_even, across_odd)
    send(0, across_even, across_even_out)
    send(1, across_odd, across_odd_out)


    def count(chunk):
        total = jnp.zeros((128, lane_count), jnp.float32)
        for r in range(rows):
            total = count_row(total, r, chunk)
        return lax.dot_general(
            jnp.ones((8, lane_count), jnp.float32),
            total,
            (((1,), (1,)), ((), ())),
            precision=lax.Precision.HIGHEST,
            preferred_element_type=jnp.float32,
        )

    for chunk in range(chunks):
        summed = count(chunk)
        if chunks == 1:
            tally[...] = jnp.broadcast_to(summed[0:1], tally.shape)
        else:
            for k in range(copies):
                tally[pl.ds(k * chunks + chunk, 1), :] = summed[0:1]
    send(2, tally, tally_out)
    for copy in sent:
        copy.wait()


def column_cells(rows, cols, c, pops, mass, flags, bubble, conversion):
    at = pl.ds(c, rows, stride=cols)
    density = pops[at, :]
    for q in range(1, LANES):
        density = density + pops[pl.ds(q * rows * cols + c, rows, stride=cols), :]
    m = mass[at, :]
    flag = flags[at, :]
    code = jnp.where(
        (flag == 1) & (conversion[at, :] == 1), FILLING, flag.astype(jnp.float32) + 1.0
    )
    return {
        MASS: m,
        FRAC: jnp.clip(m / density, 0.0, 1.0),
        CODE: code,
        BUB: bubble[at, :].astype(jnp.float32),
    }


def second_kernel(
    rows, cols, held, pops, mass, flags, bubble, conversion, across_even, across_odd,
    even_out, odd_out,
):
    state = (pops, mass, flags, bubble, conversion)

    def with_rows(low, high):
        def with_cols(left_out, right_out):
            relay(rows, cols, state, low, high, left_out, right_out)

        by_parity("gy", with_cols, even_out, odd_out)

    by_parity("gx", with_rows, across_even, across_odd)


def relay(rows, cols, state, low, high, left_out, right_out):
    tall = rows + 2
    pops = state[0]
    for out, inner_col, outer_col, sign in (
        (left_out, 0, 1, -1),
        (right_out, cols - 1, cols - 2, 1),
    ):
        for c, begin, channels in (
            (inner_col, 0, list(range(CHANNELS))),
            (outer_col, CHANNELS, outer(1, sign)),
        ):
            beside = column_cells(rows, cols, c, *state)
            for k, channel in enumerate(channels):
                out[pl.ds((begin + k) * tall + 1, rows), :] = (
                    pops[pl.ds(channel * rows * cols + c, rows, stride=cols), :]
                    if channel < LANES
                    else beside[channel]
                )
        carried = (CHANNELS + len(outer(1, sign))) * tall
        spare = carried
        for halo, row, towards in ((low, 0, 1), (high, tall - 1, -1)):
            out[pl.ds(row, CHANNELS, stride=tall), :] = halo[
                pl.ds(inner_col, CHANNELS, stride=cols), :
            ]
            for k, channel in enumerate(outer(1, sign)):
                out[pl.ds((CHANNELS + k) * tall + row, 1), :] = halo[
                    pl.ds(channel * cols + outer_col, 1), :
                ]
            beyond = outer(0, towards)
            out[pl.ds(spare, len(beyond)), :] = halo[
                pl.ds(CHANNELS * cols + inner_col, len(beyond), stride=cols), :
            ]
            spare += len(beyond)
            for channel in (heading_both(towards, sign), FRAC, CODE):
                k = beyond.index(channel)
                out[pl.ds(spare, 1), :] = halo[pl.ds((CHANNELS + k) * cols + outer_col, 1), :]
                spare += 1


def side_tiles(rows):
    tall = rows + 2
    used = (CHANNELS + 7) * tall + 2 * (7 + 3)
    return -(-used // 8) * 8


def inner_columns(cols):
    return list(range(1, cols - 1))


def edge_columns(cols):
    return [-1, 0, cols - 1, cols]


def third_kernel(rows, cols, edges, *refs):
    pops, mass_in, flags_in, bubble_in, conversion_in, across_even, across_odd = refs[:7]
    sides = refs[7:9] if edges else ()
    fixed, scaling, linear, kept, cells, near = refs[-6:]
    if not edges:
        rest, rest_table = refs[7], refs[-7]
        labels_all = rest.shape[-1]
        for chunk in range(-(-labels_all // 128)):
            here = min(128, labels_all - chunk * 128)
            rest_table[chunk, :, pl.ds(0, here)] = jnp.broadcast_to(
                rest[0:1, pl.ds(chunk * 128, here)], (8, here)
            )
    todo = edge_columns(cols) if edges else inner_columns(cols)
    stored = [c for c in todo if 0 <= c < cols]
    block = rows * cols
    tall = rows + 2
    high_rows = rows + 4
    wide = cols + 4
    total_rows = wide * high_rows

    for c in (0, 1, cols - 2, cols - 1) if edges else range(cols):
        at = pl.ds((c + 2) * high_rows + 2, rows)
        for q in range(LANES):
            cells[q, at, :] = pops[pl.ds(q * block + c, rows, stride=cols), :]
        own = column_cells(rows, cols, c, pops, mass_in, flags_in, bubble_in, conversion_in)
        for channel, value in own.items():
            cells[channel, at, :] = value

    def fill_rows(low, high):
        for halo, inner_row, outer_row, towards in (
            (low, 1, 0, 1),
            (high, high_rows - 2, high_rows - 1, -1),
        ):
            for channel in range(CHANNELS):
                cells[channel, pl.ds(2 * high_rows + inner_row, cols, stride=high_rows), :] = halo[
                    pl.ds(channel * cols, cols), :
                ]
            for k, channel in enumerate(outer(0, towards)):
                cells[channel, pl.ds(2 * high_rows + outer_row, cols, stride=high_rows), :] = halo[
                    pl.ds((CHANNELS + k) * cols, cols), :
                ]

    def fill_cols(left, right):
        for halo, inner_col, outer_col, sign in (
            (left, 1, 0, 1),
            (right, wide - 2, wide - 1, -1),
        ):
            for channel in range(CHANNELS):
                cells[channel, pl.ds(inner_col * high_rows + 1, tall), :] = halo[
                    pl.ds(channel * tall, tall), :
                ]
            for k, channel in enumerate(outer(1, sign)):
                cells[channel, pl.ds(outer_col * high_rows + 1, tall), :] = halo[
                    pl.ds((CHANNELS + k) * tall, tall), :
                ]
            spare = (CHANNELS + 7) * tall
            for row, towards in ((0, 1), (high_rows - 1, -1)):
                for channel in outer(0, towards):
                    cells[channel, pl.ds(inner_col * high_rows + row, 1), :] = halo[
                        pl.ds(spare, 1), :
                    ]
                    spare += 1
                for channel in (heading_both(towards, sign), FRAC, CODE):
                    cells[channel, pl.ds(outer_col * high_rows + row, 1), :] = halo[
                        pl.ds(spare, 1), :
                    ]
                    spare += 1

    by_parity("gx", fill_rows, across_even, across_odd)
    if edges:
        by_parity("gy", fill_cols, *sides)

    if edges:
        spans = ((0, 4 * high_rows), (total_rows - 4 * high_rows, total_rows))
    else:
        spans = ((2 * high_rows, total_rows - 2 * high_rows),)
    for begin, end in [(b, min(b + 8, e)) for low, e in spans for b in range(low, e, 8)]:
        at = pl.ds(begin, end - begin)
        code = cells[CODE, at, :]
        fraction = cells[FRAC, at, :]
        face = (code == FACE) | (code == FILLING)
        u = jnp.where(code == LIQUID, 1.0, jnp.where(face, 0.5 * fraction, 0.0))
        v = jnp.where(face, 0.5, 0.0)
        free = jnp.where(code == FACE, 1.0, 0.0)
        for depth in (-1, 0, 1):
            for k, value in enumerate((code, u, v)):
                near[k * 3 + depth + 1, at, :] = roll(value, depth) if depth else value
        ends = roll(free, 1) + roll(free, -1)
        near[9, at, :] = free
        near[10, at, :] = ends
        near[11, at, :] = free + ends

    for slot, c in enumerate(todo):
        base = (c + 2) * high_rows + 1
        inside = 0 <= c < cols
        out = pl.ds(slot * tall, tall)
        column = pl.ds(stored.index(c) * tall if inside else 0, tall)

        def source(array, q, base=base):
            begin = base - int(VELOCITIES[q][1]) * high_rows - int(VELOCITIES[q][0])
            return array[pl.ds(begin, tall), :]

        own = [cells[q, pl.ds(base, tall), :] for q in range(LANES)]
        mass = cells[MASS, pl.ds(base, tall), :]
        fraction = cells[FRAC, pl.ds(base, tall), :]
        code = cells[CODE, pl.ds(base, tall), :]
        dry = code == GAS
        density = total(own)
        inverse = 1.0 / density
        velocity = [j * inverse for j in momentum(own)]
        still = rest_part(velocity)
        flow = None
        constant = [own[0]] + [None] * (LANES - 1)
        factor = [None] * LANES
        for first in range(1, LANES, 2):
            project = projection(velocity, first)
            pressed = (2.0 * WEIGHTS[first]) * (still + 4.5 * project * project)
            for q in (first, first + 1):
                depth = int(VELOCITIES[q][2])
                moved = source(cells.at[q], q)
                if depth:
                    moved = roll(moved, depth)
                bounced = own[OPPOSITE[q]]
                kind = source(near.at[depth + 1], q)
                weight = source(near.at[3 + depth + 1], q) + source(near.at[6 + depth + 1], q) * fraction
                term = weight * (moved - bounced)
                flow = term if flow is None else flow + term
                gas_side = kind == GAS
                constant[q] = jnp.where(
                    gas_side, -bounced, jnp.where(kind == WALL, bounced, moved)
                )
                factor[q] = jnp.where(gas_side, pressed, 0.0)
        targets = near[10, pl.ds(base, tall), :]
        for dr in (-1, 0, 1):
            for dc in (-1, 0, 1):
                if dr or dc:
                    plane = 9 if dr and dc else 11
                    targets = targets + near[plane, pl.ds(base + dc * high_rows + dr, tall), :]
        linear[0, out, :] = total(constant)
        linear[1, out, :] = total(factor[1:])
        kept[0, out, :] = mass + flow
        kept[1, out, :] = jnp.maximum(targets, 1.0)
        kept[2, out, :] = code
        kept[3, out, :] = cells[BUB, pl.ds(base, tall), :]
        if inside:
            kept[4, out, :] = mass
            for axis, j in enumerate(momentum(constant)):
                linear[2 + axis, out, :] = j
            for axis, j in enumerate(momentum(factor)):
                linear[5 + axis, out, :] = j
            for q in range(LANES):
                fixed[q, column, :] = jnp.where(dry, own[q], (1.0 - RELAX) * constant[q])
                if q:
                    scaling[q - 1, column, :] = jnp.where(dry, 0.0, (1.0 - RELAX) * factor[q])


def total(tiles):
    out = tiles[0]
    for t in tiles[1:]:
        out = out + t
    return out


def momentum(tiles):
    flux = []
    for axis in range(3):
        plus = [tiles[q] for q in heading(axis, 1)]
        minus = [tiles[q] for q in heading(axis, -1)]
        j = plus[0] - minus[0]
        for a, b in zip(plus[1:], minus[1:]):
            j = j + (a - b)
        flux.append(j)
    return flux


def rest_part(velocity):
    return 1.0 - 1.5 * (
        velocity[0] * velocity[0] + velocity[1] * velocity[1] + velocity[2] * velocity[2]
    )


def projection(velocity, q):
    terms = [
        velocity[axis] if VELOCITIES[q][axis] > 0 else -velocity[axis]
        for axis in range(3)
        if VELOCITIES[q][axis]
    ]
    return total(terms)


def fourth_kernel(
    rows, cols, chunks, copies, labels,
    inner_fixed, inner_scaling, inner_linear, inner_kept,
    edge_fixed, edge_scaling, edge_linear, edge_kept, tally, rest,
    relaxed_out, new_mass_out, gas_out,
    sums, table, relaxed_stage, mass_stage, gas_stage, wet_sem, mass_sem, gas_sem,
):
    block = rows * cols
    tall = rows + 2
    for chunk in range(chunks):
        rows_of = pl.ds(chunk, copies, stride=chunks) if chunks > 1 else pl.ds(0, copies)
        volume = jnp.sum(tally[rows_of, :], axis=0, keepdims=True)
        here = min(128, labels - chunk * 128)
        gas = AMBIENT + rest[chunk] / jnp.maximum(volume, 1.0)
        gas_stage[0:1, pl.ds(chunk * 128, here)] = gas[0:1, :here]
        table[chunk] = gas
    gas_copy = pltpu.make_async_copy(gas_stage, gas_out, gas_sem)
    gas_copy.start()

    def place(c):
        if c in inner_columns(cols):
            slot = inner_columns(cols).index(c)
            parts = (inner_fixed, inner_scaling, inner_linear, inner_kept)
            return parts, pl.ds(slot * tall, tall), pl.ds(slot * tall, tall)
        slot = edge_columns(cols).index(c)
        parts = (edge_fixed, edge_scaling, edge_linear, edge_kept)
        return parts, pl.ds(slot * tall, tall), pl.ds((0 if c <= 0 else 1) * tall, tall)

    def settled(c):
        (_, _, linear, kept), at, _ = place(c)
        code = kept[2, at, :]
        bubble = kept[3, at, :].astype(jnp.int32)
        gas = None
        for chunk in range(chunks):
            index = bubble - chunk * 128
            valid = (index >= 0) & (index < 128)
            found = jnp.take_along_axis(
                table[chunk, pl.ds(0, tall), :], jnp.where(valid, index, 0), axis=1
            )
            gas = found if gas is None else jnp.where(valid, found, gas)
        density = linear[0, at, :] + gas * linear[1, at, :]
        portion = jnp.where(
            code == FILLING, (kept[0, at, :] - density) / kept[1, at, :], 0.0
        )
        return at, code, gas, density, portion

    updates, portions, states = [], [], []
    for c in range(cols):
        _, code, gas, density, portion = settled(c)
        (_, _, linear, kept), at, _ = place(c)
        portions.append(portion)
        dry = code == GAS
        updates.append(
            jnp.where(
                code == FACE,
                kept[0, at, :],
                jnp.where(dry, kept[4, at, :], density),
            )
        )
        inverse = 1.0 / jnp.where(dry, 1.0, density)
        velocity = [
            (linear[2 + axis, at, :] + gas * linear[5 + axis, at, :]) * inverse for axis in range(3)
        ]
        states.append((gas, velocity, rest_part(velocity), jnp.where(dry, 0.0, RELAX * density)))

    relaxed_copies = []

    def leave(q):
        copy = pltpu.make_async_copy(
            relaxed_stage.at[pl.ds((q * tall + 1) * cols, block), :],
            relaxed_out.at[pl.ds(q * block, block), :],
            wet_sem.at[q],
        )
        copy.start()
        relaxed_copies.append(copy)

    def put(q, c, value):
        relaxed_stage[pl.ds(q * tall * cols + c, tall, stride=cols), :] = value

    for c, (_, _, still, scaled) in enumerate(states):
        (fixed, _, _, _), _, column = place(c)
        put(0, c, fixed[0, column, :] + (scaled * WEIGHTS[0]) * still)
    leave(0)
    for first in range(1, LANES, 2):
        for c, (gas, velocity, still, scaled) in enumerate(states):
            (fixed, scaling, _, _), _, column = place(c)
            project = projection(velocity, first)
            even = still + 4.5 * project * project
            odd = 3.0 * project
            share = scaled * WEIGHTS[first]
            for q, part in ((first, even + odd), (first + 1, even - odd)):
                put(q, c, fixed[q, column, :] + gas * scaling[q - 1, column, :] + share * part)
        leave(first)
        leave(first + 1)

    portions = [settled(-1)[-1]] + portions + [settled(cols)[-1]]
    ends = [roll(p, 1) + roll(p, -1) for p in portions]
    full = [p + e for p, e in zip(portions, ends)]
    for c in range(cols):
        beside = ends[c + 1] + full[c] + full[c + 2]
        stacked = full[c + 1] + portions[c] + portions[c + 2]
        sums[pl.ds(8, tall), :] = stacked
        gained = beside + sums[pl.ds(7, tall), :] + sums[pl.ds(9, tall), :]
        (_, _, _, kept), at, _ = place(c)
        code = kept[2, at, :]
        mass_stage[pl.ds(c, tall, stride=cols), :] = jnp.where(
            code == FACE, updates[c] + gained, updates[c]
        )
    mass_copy = pltpu.make_async_copy(
        mass_stage.at[pl.ds(cols, block), :], new_mass_out, mass_sem
    )
    mass_copy.start()
    for copy in relaxed_copies:
        copy.wait()
    mass_copy.wait()
    gas_copy.wait()


def shards(gx_size, gy_size, populations, cell_mass, cell_flags, bubble, conversion, rest_volume):
    rows, cols, depth = populations.shape[1:]
    labels = rest_volume.shape[0]
    block = rows * cols
    tall = rows + 2
    devices = gx_size * gy_size
    chunks = -(-labels // 128)
    direct = devices * chunks <= 64
    copies = devices if direct else 1
    f32 = jnp.float32
    vmem = pl.BlockSpec(memory_space=pltpu.VMEM)
    hbm = pl.BlockSpec(memory_space=pltpu.HBM)

    pops = populations.reshape(LANES * block, depth)
    flat = [a.reshape(block, depth) for a in (cell_mass, cell_flags, bubble, conversion)]
    end_rows = (CHANNELS + 7) * cols
    side_rows = side_tiles(rows)

    packed = [
        (end_rows, depth),
        (end_rows, depth),
        (copies * chunks, 128),
    ]
    across_even, across_odd, tally = pl.pallas_call(
        functools.partial(first_kernel, rows, cols, chunks, copies),
        out_shape=[jax.ShapeDtypeStruct(shape, f32) for shape in packed],
        in_specs=[hbm] * 5,
        out_specs=[hbm] * len(packed),
        scratch_shapes=[
            pltpu.VMEM((4 * block, depth), f32),
            pltpu.VMEM((LANES, block, depth), f32),
            pltpu.VMEM((block, depth), f32),
            pltpu.VMEM((block, depth), jnp.int32),
            pltpu.VMEM((block, depth), jnp.int32),
            pltpu.VMEM((block, depth), jnp.int32),
            pltpu.SemaphoreType.DMA((5,)),
        ]
        + [pltpu.VMEM(shape, f32) for shape in packed]
        + [pltpu.SemaphoreType.DMA((len(packed),))],
        cost_estimate=pl.CostEstimate(flops=2000000, bytes_accessed=2000000, transcendentals=0),
        compiler_params=pltpu.CompilerParams(vmem_limit_bytes=67043328),
        name="pack",
    )(populations.reshape(LANES, block, depth), *flat)

    held = pl.pallas_call(
        lambda out: out.__setitem__(Ellipsis, jnp.zeros((8, 128), f32)),
        out_shape=jax.ShapeDtypeStruct((8, 128), f32),
        out_specs=vmem,
        cost_estimate=pl.CostEstimate(flops=HOLD, bytes_accessed=4096, transcendentals=0),
        compiler_params=pltpu.CompilerParams(vmem_limit_bytes=1 << 20),
        name="pause",
    )()

    def swapped(x, axis, size, odd):
        return lax.ppermute(x, axis, paired(size, odd))

    across_odd = swapped(across_odd, "gx", gx_size, True)
    across_even = swapped(across_even, "gx", gx_size, False)
    if direct:
        tallies = lax.all_to_all(tally, ("gx", "gy"), 0, 0, tiled=True)
    else:
        tallies = lax.psum(tally, ("gx", "gy"))

    beside_even, beside_odd = pl.pallas_call(
        functools.partial(second_kernel, rows, cols),
        out_shape=[jax.ShapeDtypeStruct((side_rows, depth), f32)] * 2,
        in_specs=[vmem] * 8,
        out_specs=[vmem] * 2,
        compiler_params=pltpu.CompilerParams(vmem_limit_bytes=4 << 20),
        name="relay",
    )(held, pops, *flat, across_even, across_odd)
    beside_odd = swapped(beside_odd, "gy", gy_size, True)
    beside_even = swapped(beside_even, "gy", gy_size, False)

    def prepare(edges, *sides):
        todo = edge_columns(cols) if edges else inner_columns(cols)
        stored = [c for c in todo if 0 <= c < cols]
        prepared = [
            (LANES, len(stored) * tall, depth),
            (LANES - 1, len(stored) * tall, depth),
            (8, len(todo) * tall, depth),
            (5, len(todo) * tall, depth),
        ]
        if not edges:
            prepared.insert(0, (chunks, 8, 128))
        return pl.pallas_call(
            functools.partial(third_kernel, rows, cols, edges),
            out_shape=[jax.ShapeDtypeStruct(shape, f32) for shape in prepared],
            in_specs=[vmem] * (7 + len(sides)),
            out_specs=[vmem] * len(prepared),
            scratch_shapes=[
                pltpu.VMEM((CHANNELS, (cols + 4) * (rows + 4), depth), f32),
                pltpu.VMEM((12, (cols + 4) * (rows + 4), depth), f32),
            ],
            cost_estimate=pl.CostEstimate(flops=5000000, bytes_accessed=3000000, transcendentals=0),
            compiler_params=pltpu.CompilerParams(vmem_limit_bytes=8 << 20),
            name="edges" if edges else "inner",
        )(pops, *flat, across_even, across_odd, *sides)

    rest, *inner = prepare(False, rest_volume.reshape(1, labels))
    edge = prepare(True, beside_even, beside_odd)
    relaxed, new_mass, gas = pl.pallas_call(
        functools.partial(fourth_kernel, rows, cols, chunks, copies, labels),
        out_shape=[
            jax.ShapeDtypeStruct((LANES * block, depth), f32),
            jax.ShapeDtypeStruct((block, depth), f32),
            jax.ShapeDtypeStruct((1, labels), f32),
        ],
        in_specs=[vmem] * 10,
        out_specs=[pl.BlockSpec(memory_space=pl.ANY)] * 3,
        scratch_shapes=[
            pltpu.VMEM((24, depth), f32),
            pltpu.VMEM((chunks, 8, 128), f32),
            pltpu.VMEM((LANES * tall * cols, depth), f32),
            pltpu.VMEM((tall * cols, depth), f32),
            pltpu.VMEM((1, labels), f32),
            pltpu.SemaphoreType.DMA((LANES,)),
            pltpu.SemaphoreType.DMA,
            pltpu.SemaphoreType.DMA,
        ],
        cost_estimate=pl.CostEstimate(flops=2000000, bytes_accessed=3000000, transcendentals=0),
        compiler_params=pltpu.CompilerParams(vmem_limit_bytes=12 << 20),
        name="settle",
    )(*inner, *edge, tallies, rest)
    return (
        relaxed.reshape(LANES, rows, cols, depth),
        new_mass.reshape(rows, cols, depth),
        gas.reshape(labels),
    )


def solution(mesh):
    placed = (
        P(None, "gx", "gy", None),
        P("gx", "gy", None),
        P("gx", "gy", None),
        P("gx", "gy", None),
        P("gx", "gy", None),
        P(),
    )

    def step(*args):
        return shards(mesh.shape["gx"], mesh.shape["gy"], *args)

    return jax.shard_map(
        step,
        mesh=mesh,
        in_specs=placed,
        out_specs=(P(None, "gx", "gy", None), P("gx", "gy", None), P()),
        check_vma=False,
    )
```

```python
import functools

import jax
import jax.numpy as jnp
import numpy as np
from jax import lax
from jax.experimental import pallas as pl
from jax.experimental.pallas import tpu as pltpu
from jax.sharding import PartitionSpec as P


VELOCITIES = np.array(
    [
        [0, 0, 0],
        [1, 0, 0],
        [-1, 0, 0],
        [0, 1, 0],
        [0, -1, 0],
        [0, 0, 1],
        [0, 0, -1],
        [1, 1, 0],
        [-1, -1, 0],
        [1, -1, 0],
        [-1, 1, 0],
        [1, 0, 1],
        [-1, 0, -1],
        [1, 0, -1],
        [-1, 0, 1],
        [0, 1, 1],
        [0, -1, -1],
        [0, 1, -1],
        [0, -1, 1],
    ]
)
OPPOSITE = [0, 2, 1, 4, 3, 6, 5, 8, 7, 10, 9, 12, 11, 14, 13, 16, 15, 18, 17]
WEIGHTS = [1.0 / 3.0] + [1.0 / 18.0] * 6 + [1.0 / 36.0] * 12
RELAX = 1.0 / 0.6
AMBIENT = 2.0
HOLD = 2000000000
LANES = 19
MASS, FRAC, CODE, BUB = 19, 20, 21, 22
CHANNELS = 23
WALL, GAS, FACE, LIQUID, FILLING = 0.0, 1.0, 2.0, 3.0, 5.0


def heading(axis, sign):
    return [q for q in range(LANES) if VELOCITIES[q][axis] == sign]


def heading_both(rows, cols):
    return [q for q in range(LANES) if VELOCITIES[q][0] == rows and VELOCITIES[q][1] == cols][0]


def outer(axis, sign):
    return heading(axis, sign) + [FRAC, CODE]


def roll(x, shift):
    return pltpu.roll(x, shift % x.shape[-1], x.ndim - 1)


def by_parity(axis, use, even, odd):
    odd_device = lax.rem(lax.axis_index(axis), 2) == 1

    @pl.when(odd_device)
    def _():
        use(even, odd)

    @pl.when(jnp.logical_not(odd_device))
    def _():
        use(odd, even)


def paired(size, odd):
    pairs = []
    for i in range(1 if odd else 0, size - 1, 2):
        pairs += [(i, i + 1), (i + 1, i)]
    return pairs


def first_kernel(
    rows, cols, chunks, copies, label_span,
    pops_in, mass_in, flags_in, bubble_in, conversion_in,
    across_even_out, across_odd_out, tally_out,
    aux, pops, mass, flags, bubble, conversion, sems,
    across_even, across_odd, tally, out_sems,
):
    block = rows * cols
    copies_in = [
        pltpu.make_async_copy(a, b, sems.at[k])
        for k, (a, b) in enumerate(
            (
                (pops_in, pops),
                (mass_in, mass),
                (flags_in, flags),
                (bubble_in, bubble),
                (conversion_in, conversion),
            )
        )
    ]
    for copy in copies_in:
        copy.start()
    for copy in copies_in:
        copy.wait()
    sent = []

    def send(k, staged, out):
        copy = pltpu.make_async_copy(staged, out, out_sems.at[k])
        copy.start()
        sent.append(copy)

    contributions = []
    lane_count = mass.shape[-1]
    tall_labels = 128 if chunks > 1 else label_span
    label_rows = lax.broadcasted_iota(jnp.int32, (tall_labels, lane_count), 0)

    def count_row(total, r, chunk):
        for c in range(cols):
            row = bubble[pl.ds(r * cols + c, 1), :]
            term = contributions[r][c : c + 1, :]
            total = total + jnp.where(label_rows + chunk * 128 == row, term, 0.0)
        return total

    for r in range(rows):
        at = pl.ds(r * cols, cols)
        density = pops[0, at, :]
        for q in range(1, LANES):
            density = density + pops[q, at, :]
        m = mass[at, :]
        flag = flags[at, :]
        fraction = jnp.clip(m / density, 0.0, 1.0)
        code = jnp.where(
            (flag == 1) & (conversion[at, :] == 1), FILLING, flag.astype(jnp.float32) + 1.0
        )
        aux[at, :] = m
        aux[pl.ds(block + r * cols, cols), :] = fraction
        aux[pl.ds(2 * block + r * cols, cols), :] = code
        aux[pl.ds(3 * block + r * cols, cols), :] = bubble[at, :].astype(jnp.float32)
        contributions.append(
            jnp.where(flag == 0, 1.0, jnp.where(flag == 1, 1.0 - fraction, 0.0))
        )

    def tile(channel, r):
        if channel < LANES:
            return pops[channel, pl.ds(r * cols, cols), :]
        return aux[pl.ds((channel - LANES) * block + r * cols, cols), :]

    def send_rows(out, inner_row, outer_row, sign):
        for channel in range(CHANNELS):
            out[pl.ds(channel * cols, cols), :] = tile(channel, inner_row)
        for k, channel in enumerate(outer(0, sign)):
            out[pl.ds((CHANNELS + k) * cols, cols), :] = tile(channel, outer_row)

    def low_high(low, high):
        send_rows(low, 0, 1, -1)
        send_rows(high, rows - 1, rows - 2, 1)

    by_parity("gx", low_high, across_even, across_odd)
    send(0, across_even, across_even_out)
    send(1, across_odd, across_odd_out)


    def count(chunk):
        total = jnp.zeros((tall_labels, lane_count), jnp.float32)
        for r in range(rows):
            total = count_row(total, r, chunk)
        high = total.astype(jnp.bfloat16)
        left = total - high.astype(jnp.float32)
        middle = left.astype(jnp.bfloat16)
        low = (left - middle.astype(jnp.float32)).astype(jnp.bfloat16)
        return lax.dot_general(
            jnp.ones((16, 3 * lane_count), jnp.bfloat16),
            jnp.concatenate([high, middle, low], axis=1),
            (((1,), (1,)), ((), ())),
            preferred_element_type=jnp.float32,
        )

    for chunk in range(chunks):
        summed = count(chunk)
        if chunks == 1:
            tally[...] = jnp.zeros(tally.shape, jnp.float32)
            tally[:, pl.ds(0, tall_labels)] = jnp.broadcast_to(summed[0:1], (copies, tall_labels))
        else:
            for k in range(copies):
                tally[pl.ds(k * chunks + chunk, 1), :] = summed[0:1]
    send(2, tally, tally_out)
    for copy in sent:
        copy.wait()


def column_cells(rows, cols, c, pops, mass, flags, bubble, conversion):
    at = pl.ds(c, rows, stride=cols)
    density = pops[at, :]
    for q in range(1, LANES):
        density = density + pops[pl.ds(q * rows * cols + c, rows, stride=cols), :]
    m = mass[at, :]
    flag = flags[at, :]
    code = jnp.where(
        (flag == 1) & (conversion[at, :] == 1), FILLING, flag.astype(jnp.float32) + 1.0
    )
    return {
        MASS: m,
        FRAC: jnp.clip(m / density, 0.0, 1.0),
        CODE: code,
        BUB: bubble[at, :].astype(jnp.float32),
    }


def second_kernel(
    rows, cols, held, pops, mass, flags, bubble, conversion, across_even, across_odd,
    even_out, odd_out,
):
    state = (pops, mass, flags, bubble, conversion)

    def with_rows(low, high):
        def with_cols(left_out, right_out):
            relay(rows, cols, state, low, high, left_out, right_out)

        by_parity("gy", with_cols, even_out, odd_out)

    by_parity("gx", with_rows, across_even, across_odd)


def relay(rows, cols, state, low, high, left_out, right_out):
    tall = rows + 2
    pops = state[0]
    for out, inner_col, outer_col, sign in (
        (left_out, 0, 1, -1),
        (right_out, cols - 1, cols - 2, 1),
    ):
        for c, begin, channels in (
            (inner_col, 0, list(range(CHANNELS))),
            (outer_col, CHANNELS, outer(1, sign)),
        ):
            beside = column_cells(rows, cols, c, *state)
            for k, channel in enumerate(channels):
                out[pl.ds((begin + k) * tall + 1, rows), :] = (
                    pops[pl.ds(channel * rows * cols + c, rows, stride=cols), :]
                    if channel < LANES
                    else beside[channel]
                )
        carried = (CHANNELS + len(outer(1, sign))) * tall
        spare = carried
        for halo, row, towards in ((low, 0, 1), (high, tall - 1, -1)):
            out[pl.ds(row, CHANNELS, stride=tall), :] = halo[
                pl.ds(inner_col, CHANNELS, stride=cols), :
            ]
            for k, channel in enumerate(outer(1, sign)):
                out[pl.ds((CHANNELS + k) * tall + row, 1), :] = halo[
                    pl.ds(channel * cols + outer_col, 1), :
                ]
            beyond = outer(0, towards)
            out[pl.ds(spare, len(beyond)), :] = halo[
                pl.ds(CHANNELS * cols + inner_col, len(beyond), stride=cols), :
            ]
            spare += len(beyond)
            for channel in (heading_both(towards, sign), FRAC, CODE):
                k = beyond.index(channel)
                out[pl.ds(spare, 1), :] = halo[pl.ds((CHANNELS + k) * cols + outer_col, 1), :]
                spare += 1


def side_tiles(rows):
    tall = rows + 2
    used = (CHANNELS + 7) * tall + 2 * (7 + 3)
    return -(-used // 8) * 8


def inner_columns(cols):
    return list(range(1, cols - 1))


def edge_columns(cols):
    return [-1, 0, cols - 1, cols]


def third_kernel(rows, cols, edges, *refs):
    pops, mass_in, flags_in, bubble_in, conversion_in, across_even, across_odd = refs[:7]
    sides = refs[7:9] if edges else ()
    fixed, scaling, linear, kept, cells, near = refs[-6:]
    if not edges:
        rest, rest_table = refs[7], refs[-7]
        labels_all = rest.shape[-1]
        for chunk in range(-(-labels_all // 128)):
            here = min(128, labels_all - chunk * 128)
            rest_table[chunk, :, pl.ds(0, here)] = jnp.broadcast_to(
                rest[0:1, pl.ds(chunk * 128, here)], (8, here)
            )
    todo = edge_columns(cols) if edges else inner_columns(cols)
    stored = [c for c in todo if 0 <= c < cols]
    block = rows * cols
    tall = rows + 2
    high_rows = rows + 4
    wide = cols + 4
    total_rows = wide * high_rows

    for c in (0, 1, cols - 2, cols - 1) if edges else range(cols):
        at = pl.ds((c + 2) * high_rows + 2, rows)
        for q in range(LANES):
            cells[q, at, :] = pops[pl.ds(q * block + c, rows, stride=cols), :]
        own = column_cells(rows, cols, c, pops, mass_in, flags_in, bubble_in, conversion_in)
        for channel, value in own.items():
            cells[channel, at, :] = value

    def fill_rows(low, high):
        for halo, inner_row, outer_row, towards in (
            (low, 1, 0, 1),
            (high, high_rows - 2, high_rows - 1, -1),
        ):
            for channel in range(CHANNELS):
                cells[channel, pl.ds(2 * high_rows + inner_row, cols, stride=high_rows), :] = halo[
                    pl.ds(channel * cols, cols), :
                ]
            for k, channel in enumerate(outer(0, towards)):
                cells[channel, pl.ds(2 * high_rows + outer_row, cols, stride=high_rows), :] = halo[
                    pl.ds((CHANNELS + k) * cols, cols), :
                ]

    def fill_cols(left, right):
        for halo, inner_col, outer_col, sign in (
            (left, 1, 0, 1),
            (right, wide - 2, wide - 1, -1),
        ):
            for channel in range(CHANNELS):
                cells[channel, pl.ds(inner_col * high_rows + 1, tall), :] = halo[
                    pl.ds(channel * tall, tall), :
                ]
            for k, channel in enumerate(outer(1, sign)):
                cells[channel, pl.ds(outer_col * high_rows + 1, tall), :] = halo[
                    pl.ds((CHANNELS + k) * tall, tall), :
                ]
            spare = (CHANNELS + 7) * tall
            for row, towards in ((0, 1), (high_rows - 1, -1)):
                for channel in outer(0, towards):
                    cells[channel, pl.ds(inner_col * high_rows + row, 1), :] = halo[
                        pl.ds(spare, 1), :
                    ]
                    spare += 1
                for channel in (heading_both(towards, sign), FRAC, CODE):
                    cells[channel, pl.ds(outer_col * high_rows + row, 1), :] = halo[
                        pl.ds(spare, 1), :
                    ]
                    spare += 1

    by_parity("gx", fill_rows, across_even, across_odd)
    if edges:
        by_parity("gy", fill_cols, *sides)

    if edges:
        spans = ((0, 4 * high_rows), (total_rows - 4 * high_rows, total_rows))
    else:
        spans = ((2 * high_rows, total_rows - 2 * high_rows),)
    for begin, end in [(b, min(b + 8, e)) for low, e in spans for b in range(low, e, 8)]:
        at = pl.ds(begin, end - begin)
        code = cells[CODE, at, :]
        fraction = cells[FRAC, at, :]
        face = (code == FACE) | (code == FILLING)
        u = jnp.where(code == LIQUID, 1.0, jnp.where(face, 0.5 * fraction, 0.0))
        v = jnp.where(face, 0.5, 0.0)
        free = jnp.where(code == FACE, 1.0, 0.0)
        for depth in (-1, 0, 1):
            for k, value in enumerate((code, u, v)):
                near[k * 3 + depth + 1, at, :] = roll(value, depth) if depth else value
        ends = roll(free, 1) + roll(free, -1)
        near[9, at, :] = free
        near[10, at, :] = ends
        near[11, at, :] = free + ends

    for slot, c in enumerate(todo):
        base = (c + 2) * high_rows + 1
        inside = 0 <= c < cols
        out = pl.ds(slot * tall, tall)
        column = pl.ds(stored.index(c) * tall if inside else 0, tall)

        def source(array, q, base=base):
            begin = base - int(VELOCITIES[q][1]) * high_rows - int(VELOCITIES[q][0])
            return array[pl.ds(begin, tall), :]

        own = [cells[q, pl.ds(base, tall), :] for q in range(LANES)]
        mass = cells[MASS, pl.ds(base, tall), :]
        fraction = cells[FRAC, pl.ds(base, tall), :]
        code = cells[CODE, pl.ds(base, tall), :]
        dry = code == GAS
        density = total(own)
        inverse = 1.0 / density
        velocity = [j * inverse for j in momentum(own)]
        still = rest_part(velocity)
        flow = None
        constant = [own[0]] + [None] * (LANES - 1)
        factor = [None] * LANES
        for first in range(1, LANES, 2):
            project = projection(velocity, first)
            pressed = (2.0 * WEIGHTS[first]) * (still + 4.5 * project * project)
            for q in (first, first + 1):
                depth = int(VELOCITIES[q][2])
                moved = source(cells.at[q], q)
                if depth:
                    moved = roll(moved, depth)
                bounced = own[OPPOSITE[q]]
                kind = source(near.at[depth + 1], q)
                weight = source(near.at[3 + depth + 1], q) + source(near.at[6 + depth + 1], q) * fraction
                term = weight * (moved - bounced)
                flow = term if flow is None else flow + term
                gas_side = kind == GAS
                constant[q] = jnp.where(
                    gas_side, -bounced, jnp.where(kind == WALL, bounced, moved)
                )
                factor[q] = jnp.where(gas_side, pressed, 0.0)
        targets = near[10, pl.ds(base, tall), :]
        for dr in (-1, 0, 1):
            for dc in (-1, 0, 1):
                if dr or dc:
                    plane = 9 if dr and dc else 11
                    targets = targets + near[plane, pl.ds(base + dc * high_rows + dr, tall), :]
        linear[0, out, :] = total(constant)
        linear[1, out, :] = total(factor[1:])
        kept[0, out, :] = mass + flow
        kept[1, out, :] = jnp.maximum(targets, 1.0)
        kept[2, out, :] = code
        kept[3, out, :] = cells[BUB, pl.ds(base, tall), :]
        if inside:
            kept[4, out, :] = mass
            for axis, j in enumerate(momentum(constant)):
                linear[2 + axis, out, :] = j
            for axis, j in enumerate(momentum(factor)):
                linear[5 + axis, out, :] = j
            for q in range(LANES):
                fixed[q, column, :] = jnp.where(dry, own[q], (1.0 - RELAX) * constant[q])
                if q:
                    scaling[q - 1, column, :] = jnp.where(dry, 0.0, (1.0 - RELAX) * factor[q])


def total(tiles):
    out = tiles[0]
    for t in tiles[1:]:
        out = out + t
    return out


def momentum(tiles):
    flux = []
    for axis in range(3):
        plus = [tiles[q] for q in heading(axis, 1)]
        minus = [tiles[q] for q in heading(axis, -1)]
        j = plus[0] - minus[0]
        for a, b in zip(plus[1:], minus[1:]):
            j = j + (a - b)
        flux.append(j)
    return flux


def rest_part(velocity):
    return 1.0 - 1.5 * (
        velocity[0] * velocity[0] + velocity[1] * velocity[1] + velocity[2] * velocity[2]
    )


def projection(velocity, q):
    terms = [
        velocity[axis] if VELOCITIES[q][axis] > 0 else -velocity[axis]
        for axis in range(3)
        if VELOCITIES[q][axis]
    ]
    return total(terms)


def fourth_kernel(
    rows, cols, chunks, copies, labels,
    inner_fixed, inner_scaling, inner_linear, inner_kept,
    edge_fixed, edge_scaling, edge_linear, edge_kept, tally, rest,
    relaxed_out, new_mass_out, gas_out,
    sums, table, relaxed_stage, mass_stage, gas_stage, wet_sem, mass_sem, gas_sem,
):
    block = rows * cols
    tall = rows + 2
    for chunk in range(chunks):
        rows_of = pl.ds(chunk, copies, stride=chunks) if chunks > 1 else pl.ds(0, copies)
        volume = jnp.sum(tally[rows_of, :], axis=0, keepdims=True)
        here = min(128, labels - chunk * 128)
        gas = AMBIENT + rest[chunk] / jnp.maximum(volume, 1.0)
        gas_stage[0:1, pl.ds(chunk * 128, here)] = gas[0:1, :here]
        table[chunk] = gas
    gas_copy = pltpu.make_async_copy(gas_stage, gas_out, gas_sem)
    gas_copy.start()

    def place(c):
        if c in inner_columns(cols):
            slot = inner_columns(cols).index(c)
            parts = (inner_fixed, inner_scaling, inner_linear, inner_kept)
            return parts, pl.ds(slot * tall, tall), pl.ds(slot * tall, tall)
        slot = edge_columns(cols).index(c)
        parts = (edge_fixed, edge_scaling, edge_linear, edge_kept)
        return parts, pl.ds(slot * tall, tall), pl.ds((0 if c <= 0 else 1) * tall, tall)

    def settled(c):
        (_, _, linear, kept), at, _ = place(c)
        code = kept[2, at, :]
        bubble = kept[3, at, :].astype(jnp.int32)
        gas = None
        for chunk in range(chunks):
            index = bubble - chunk * 128
            valid = (index >= 0) & (index < 128)
            found = jnp.take_along_axis(
                table[chunk, pl.ds(0, tall), :], jnp.where(valid, index, 0), axis=1
            )
            gas = found if gas is None else jnp.where(valid, found, gas)
        density = linear[0, at, :] + gas * linear[1, at, :]
        portion = jnp.where(
            code == FILLING, (kept[0, at, :] - density) / kept[1, at, :], 0.0
        )
        return at, code, gas, density, portion

    updates, portions, states = [], [], []
    for c in range(cols):
        _, code, gas, density, portion = settled(c)
        (_, _, linear, kept), at, _ = place(c)
        portions.append(portion)
        dry = code == GAS
        updates.append(
            jnp.where(
                code == FACE,
                kept[0, at, :],
                jnp.where(dry, kept[4, at, :], density),
            )
        )
        inverse = 1.0 / jnp.where(dry, 1.0, density)
        velocity = [
            (linear[2 + axis, at, :] + gas * linear[5 + axis, at, :]) * inverse for axis in range(3)
        ]
        states.append((gas, velocity, rest_part(velocity), jnp.where(dry, 0.0, RELAX * density)))

    portions = [settled(-1)[-1]] + portions + [settled(cols)[-1]]
    ends = [roll(p, 1) + roll(p, -1) for p in portions]
    full = [p + e for p, e in zip(portions, ends)]
    for c in range(cols):
        beside = ends[c + 1] + full[c] + full[c + 2]
        stacked = full[c + 1] + portions[c] + portions[c + 2]
        sums[pl.ds(8, tall), :] = stacked
        gained = beside + sums[pl.ds(7, tall), :] + sums[pl.ds(9, tall), :]
        (_, _, _, kept), at, _ = place(c)
        code = kept[2, at, :]
        mass_stage[pl.ds(c, tall, stride=cols), :] = jnp.where(
            code == FACE, updates[c] + gained, updates[c]
        )
    mass_copy = pltpu.make_async_copy(
        mass_stage.at[pl.ds(cols, block), :], new_mass_out, mass_sem
    )
    mass_copy.start()
    relaxed_copies = []

    def leave(q):
        copy = pltpu.make_async_copy(
            relaxed_stage.at[pl.ds((q * tall + 1) * cols, block), :],
            relaxed_out.at[pl.ds(q * block, block), :],
            wet_sem.at[q],
        )
        copy.start()
        relaxed_copies.append(copy)

    def put(q, c, value):
        relaxed_stage[pl.ds(q * tall * cols + c, tall, stride=cols), :] = value

    for c, (_, _, still, scaled) in enumerate(states):
        (fixed, _, _, _), _, column = place(c)
        put(0, c, fixed[0, column, :] + (scaled * WEIGHTS[0]) * still)
    leave(0)
    for first in range(1, LANES, 2):
        for c, (gas, velocity, still, scaled) in enumerate(states):
            (fixed, scaling, _, _), _, column = place(c)
            project = projection(velocity, first)
            even = still + 4.5 * project * project
            odd = 3.0 * project
            share = scaled * WEIGHTS[first]
            for q, part in ((first, even + odd), (first + 1, even - odd)):
                put(q, c, fixed[q, column, :] + gas * scaling[q - 1, column, :] + share * part)
        leave(first)
        leave(first + 1)

    for copy in relaxed_copies:
        copy.wait()
    mass_copy.wait()
    gas_copy.wait()


def shards(gx_size, gy_size, populations, cell_mass, cell_flags, bubble, conversion, rest_volume):
    rows, cols, depth = populations.shape[1:]
    labels = rest_volume.shape[0]
    block = rows * cols
    tall = rows + 2
    devices = gx_size * gy_size
    chunks = -(-labels // 128)
    direct = devices * chunks <= 64
    copies = devices if direct else 1
    f32 = jnp.float32
    vmem = pl.BlockSpec(memory_space=pltpu.VMEM)
    hbm = pl.BlockSpec(memory_space=pltpu.HBM)

    pops = populations.reshape(LANES * block, depth)
    flat = [a.reshape(block, depth) for a in (cell_mass, cell_flags, bubble, conversion)]
    end_rows = (CHANNELS + 7) * cols
    side_rows = side_tiles(rows)

    packed = [
        (end_rows, depth),
        (end_rows, depth),
        (copies * chunks, 128),
    ]
    across_even, across_odd, tally = pl.pallas_call(
        functools.partial(first_kernel, rows, cols, chunks, copies, min(128, -(-labels // 8) * 8)),
        out_shape=[jax.ShapeDtypeStruct(shape, f32) for shape in packed],
        in_specs=[hbm] * 5,
        out_specs=[hbm] * len(packed),
        scratch_shapes=[
            pltpu.VMEM((4 * block, depth), f32),
            pltpu.VMEM((LANES, block, depth), f32),
            pltpu.VMEM((block, depth), f32),
            pltpu.VMEM((block, depth), jnp.int32),
            pltpu.VMEM((block, depth), jnp.int32),
            pltpu.VMEM((block, depth), jnp.int32),
            pltpu.SemaphoreType.DMA((5,)),
        ]
        + [pltpu.VMEM(shape, f32) for shape in packed]
        + [pltpu.SemaphoreType.DMA((len(packed),))],
        cost_estimate=pl.CostEstimate(flops=2000000, bytes_accessed=2000000, transcendentals=0),
        compiler_params=pltpu.CompilerParams(vmem_limit_bytes=67043328),
        name="pack",
    )(populations.reshape(LANES, block, depth), *flat)

    held = pl.pallas_call(
        lambda out: out.__setitem__(Ellipsis, jnp.zeros((8, 128), f32)),
        out_shape=jax.ShapeDtypeStruct((8, 128), f32),
        out_specs=vmem,
        cost_estimate=pl.CostEstimate(flops=HOLD, bytes_accessed=4096, transcendentals=0),
        compiler_params=pltpu.CompilerParams(vmem_limit_bytes=1 << 20),
        name="pause",
    )()

    def swapped(x, axis, size, odd):
        return lax.ppermute(x, axis, paired(size, odd))

    across_odd = swapped(across_odd, "gx", gx_size, True)
    across_even = swapped(across_even, "gx", gx_size, False)
    if direct:
        tallies = lax.all_to_all(tally, ("gx", "gy"), 0, 0, tiled=True)
    else:
        tallies = lax.psum(tally, ("gx", "gy"))

    beside_even, beside_odd = pl.pallas_call(
        functools.partial(second_kernel, rows, cols),
        out_shape=[jax.ShapeDtypeStruct((side_rows, depth), f32)] * 2,
        in_specs=[vmem] * 8,
        out_specs=[vmem] * 2,
        compiler_params=pltpu.CompilerParams(vmem_limit_bytes=4 << 20),
        name="relay",
    )(held, pops, *flat, across_even, across_odd)
    beside_odd = swapped(beside_odd, "gy", gy_size, True)
    beside_even = swapped(beside_even, "gy", gy_size, False)

    def prepare(edges, *sides):
        todo = edge_columns(cols) if edges else inner_columns(cols)
        stored = [c for c in todo if 0 <= c < cols]
        prepared = [
            (LANES, len(stored) * tall, depth),
            (LANES - 1, len(stored) * tall, depth),
            (8, len(todo) * tall, depth),
            (5, len(todo) * tall, depth),
        ]
        if not edges:
            prepared.insert(0, (chunks, 8, 128))
        return pl.pallas_call(
            functools.partial(third_kernel, rows, cols, edges),
            out_shape=[jax.ShapeDtypeStruct(shape, f32) for shape in prepared],
            in_specs=[vmem] * (7 + len(sides)),
            out_specs=[vmem] * len(prepared),
            scratch_shapes=[
                pltpu.VMEM((CHANNELS, (cols + 4) * (rows + 4), depth), f32),
                pltpu.VMEM((12, (cols + 4) * (rows + 4), depth), f32),
            ],
            cost_estimate=pl.CostEstimate(flops=5000000, bytes_accessed=3000000, transcendentals=0),
            compiler_params=pltpu.CompilerParams(vmem_limit_bytes=8 << 20),
            name="edges" if edges else "inner",
        )(pops, *flat, across_even, across_odd, *sides)

    rest, *inner = prepare(False, rest_volume.reshape(1, labels))
    edge = prepare(True, beside_even, beside_odd)
    relaxed, new_mass, gas = pl.pallas_call(
        functools.partial(fourth_kernel, rows, cols, chunks, copies, labels),
        out_shape=[
            jax.ShapeDtypeStruct((LANES * block, depth), f32),
            jax.ShapeDtypeStruct((block, depth), f32),
            jax.ShapeDtypeStruct((1, labels), f32),
        ],
        in_specs=[vmem] * 10,
        out_specs=[pl.BlockSpec(memory_space=pl.ANY)] * 3,
        scratch_shapes=[
            pltpu.VMEM((24, depth), f32),
            pltpu.VMEM((chunks, 8, 128), f32),
            pltpu.VMEM((LANES * tall * cols, depth), f32),
            pltpu.VMEM((tall * cols, depth), f32),
            pltpu.VMEM((1, labels), f32),
            pltpu.SemaphoreType.DMA((LANES,)),
            pltpu.SemaphoreType.DMA,
            pltpu.SemaphoreType.DMA,
        ],
        cost_estimate=pl.CostEstimate(flops=2000000, bytes_accessed=3000000, transcendentals=0),
        compiler_params=pltpu.CompilerParams(vmem_limit_bytes=12 << 20),
        name="settle",
    )(*inner, *edge, tallies, rest)
    return (
        relaxed.reshape(LANES, rows, cols, depth),
        new_mass.reshape(rows, cols, depth),
        gas.reshape(labels),
    )


def solution(mesh):
    placed = (
        P(None, "gx", "gy", None),
        P("gx", "gy", None),
        P("gx", "gy", None),
        P("gx", "gy", None),
        P("gx", "gy", None),
        P(),
    )

    def step(*args):
        return shards(mesh.shape["gx"], mesh.shape["gy"], *args)

    return jax.shard_map(
        step,
        mesh=mesh,
        in_specs=placed,
        out_specs=(P(None, "gx", "gy", None), P("gx", "gy", None), P()),
        check_vma=False,
    )
```
